32 devices in a mesh: gx: 2 (over x), gy: 4 (over z), gz: 4 (over y, core).
Axes of the slice: x: 2, y: 2, z: 4, core: 2. Of those that a mesh axis runs over, the one named last changes fastest.
Arguments:
- point_frac: float32 [3, 131072], P(None, ('gx', 'gy', 'gz')), may hold values from 0.5 to 1.5
- cell_offset: int32 [3, 131072], P(None, ('gx', 'gy', 'gz')), may hold values from 0 to 3
- point_velocity: float32 [3, 131072], P(None, ('gx', 'gy', 'gz')), may hold values from -6 to 6
- point_affine: float32 [9, 131072], P(None, ('gx', 'gy', 'gz')), may hold values from -3 to 3
- point_stress: float32 [6, 131072], P(None, ('gx', 'gy', 'gz')), may hold values from -9.5 to 3, as said below
- point_mass: float32 [131072], P(('gx', 'gy', 'gz')), may hold values from 0.5 to 2
- block_tile: int32 [1024], P(('gx', 'gy', 'gz')), may hold values from 0 to 511, as said below
- block_count: int32 [1024], P(('gx', 'gy', 'gz')), may hold values from 1 to 128, as said below
Outputs:
- new_velocity: float32 [3, 131072], P(None, ('gx', 'gy', 'gz'))
- new_affine: float32 [9, 131072], P(None, ('gx', 'gy', 'gz'))
- new_stress: float32 [6, 131072], P(None, ('gx', 'gy', 'gz'))
- grid_velocity: float32 [3, 32, 256, 128], P(None, 'gx', 'gy', 'gz')
The draws below stay inside these ranges and needn't reach their ends.
Inputs may be any that keep to these rules, and one draw needn't show every extreme that they name: `block_tile`: block b lies on the device numbered b // 32 (gz fastest, then gy, then gx) and names a tile of that device's region, t = (tx 64 / 4 + ty) * 8 + tz; a tile may be named by no block or by several. The first block_count slots of a block hold live points. `point_stress`: components in the order xx, yy, zz, yz, xz, xy.
All inputs are finite; a program needn't handle non-finite values.
Results may differ from the reference program's by a relative error of at most 0.0003.
Values sent between devices are 32-bit elements; how exact they have to be, the bound alone decides.
No kernel may reach another device: no remote copies, remote signals or barrier semaphores. Data moves between devices by JAX's collectives and lax.ppermute only.
A program may use at most 128 MiB of HBM per device.

```python
import math
import jax
import jax.numpy as jnp
from jax import lax

CX = 16
CY = 64
CZ = 32
BLOCK = 128
B_DEV = 32
TILES_DEV = 512
BLOCKS = 1024
POINTS = 131072
NX = 32
NY = 256
NZ = 128
N_GY = 4
N_GZ = 4
DEVICES = 32


def draw_point_stress(key, part):
    subkeys = jax.random.split(key, 2)
    pressure = jnp.exp(jax.random.uniform(subkeys[0], (POINTS,), jnp.float32, math.log(0.5), math.log(8.0)))
    spread = jnp.clip(jax.random.normal(subkeys[1], (6, POINTS), jnp.float32), -3.0, 3.0)
    scales = jnp.array([0.5, 0.5, 0.5, 1.0, 1.0, 1.0], jnp.float32)
    diagonal_pick = jnp.array([1.0, 1.0, 1.0, 0.0, 0.0, 0.0], jnp.float32)
    return spread * scales[:, None] - pressure[None, :] * diagonal_pick[:, None]


def draw_block_tile(key, part):
    subkeys = jax.random.split(key, 2)
    first_draw = jax.random.randint(subkeys[0], (BLOCKS,), 0, TILES_DEV)
    second_draw = jax.random.randint(subkeys[1], (BLOCKS,), 0, TILES_DEV)
    skewed = first_draw * (second_draw + 1) // TILES_DEV
    position = jnp.arange(BLOCKS, dtype=jnp.int32)
    return jnp.where(position % B_DEV == 1, TILES_DEV - 1, skewed).astype(jnp.int32)


def draw_block_count(key, part):
    counts_drawn = jax.random.randint(key, (BLOCKS,), 1, BLOCK + 1)
    position = jnp.arange(BLOCKS, dtype=jnp.int32)
    return jnp.where(position % 64 == 0, BLOCK, counts_drawn).astype(jnp.int32)


def with_ends(entries, rng, smallest, largest):
    longest = entries.shape.index(max(entries.shape))
    spots = []
    for shift in (0, 1):
        where = [jax.random.randint(jax.random.fold_in(rng, axis), (), 0, length) for axis, length in enumerate(entries.shape)]
        where[longest] = (where[longest] + shift) % entries.shape[longest]
        spots.append(tuple(where))
    return entries.at[spots[0]].set(smallest).at[spots[1]].set(largest)


def shard_levels(own_key, shape, pieces, smallest, high):
    def one(axis_at, shards_of):
        steps = jax.random.uniform(jax.random.fold_in(jax.random.fold_in(own_key, 6), axis_at), (shards_of,), jnp.float32, smallest / len(pieces), high / len(pieces))
        return jnp.repeat(jnp.exp(steps), shape[axis_at] // shards_of).reshape((-1,) + (1,) * (len(shape) - axis_at - 1))

    loudness = one(*pieces[0])
    for cut in pieces[1:]:
        loudness = loudness * one(*cut)
    return loudness


def centred(key, extent, width, bound, cuts=(), kind=jnp.bfloat16):
    drawn = width * jax.random.normal(key, extent, jnp.float32)
    if cuts:
        drawn = drawn * shard_levels(key, extent, cuts, -0.22, 0.18)
    return jnp.clip(drawn, -bound, bound).astype(kind)


def setup_inputs(seed: int = 0) -> dict:
    key_of = jax.random.split(jax.random.key(seed), 9)
    return {
        "point_frac": jnp.clip(0.5 + 1.0 * jax.random.uniform(key_of[0], (3, POINTS), jnp.float32) ** shard_levels(key_of[0], (3, POINTS), ((1, 32),), -0.2, 0.2), 0.5, 1.5),
        "cell_offset": with_ends(jax.random.randint(key_of[1], (3, POINTS), 0, 4), jax.random.fold_in(key_of[1], 1), 0, 3).astype(jnp.int32),
        "point_velocity": centred(key_of[2], (3, POINTS), 1.0, 6.0, ((1, 32),), jnp.float32),
        "point_affine": centred(key_of[3], (9, POINTS), 0.5, 3.0, ((1, 32),), jnp.float32),
        "point_stress": draw_point_stress(jax.random.fold_in(key_of[8], 71), 0),
        "point_mass": jnp.clip(jnp.exp(math.log(2.0) - 1.3862944 * jax.random.uniform(key_of[5], (POINTS,), jnp.float32) ** shard_levels(key_of[5], (POINTS,), ((0, 32),), -0.2, 0.2)), 0.5, 2.0),
        "block_tile": draw_block_tile(jax.random.fold_in(key_of[8], 71), 0),
        "block_count": draw_block_count(jax.random.fold_in(key_of[8], 71), 0),
    }


time_step = 0.1
gravity = 1.0
shear_modulus = 2.0
bulk_modulus = 4.0
friction_static = 0.38
friction_limit = 0.64
inertial_ref = 0.28
grain_size = 0.5
grain_density = 1.0
pressure_floor = 0.5
shear_floor = 0.5
mass_floor = 0.05
stress_scale = 0.4
pair_index = ((0, 5, 4), (5, 1, 3), (4, 3, 2))
component_pairs = ((0, 0), (1, 1), (2, 2), (1, 2), (0, 2), (0, 1))

def stress_update(stress, affine):
    strain_rate = [[0.5 * (affine[3 * row_dim + col_dim] + affine[3 * col_dim + row_dim]) for col_dim in range(3)] for row_dim in range(3)]
    volume_rate = strain_rate[0][0] + strain_rate[1][1] + strain_rate[2][2]
    deviator = [[strain_rate[row_dim][col_dim] - (volume_rate / 3.0 if row_dim == col_dim else 0.0) for col_dim in range(3)] for row_dim in range(3)]
    trial_stress = []
    for component in range(6):
        row_dim, col_dim = component_pairs[component]
        value = stress[component] + time_step * 2.0 * shear_modulus * deviator[row_dim][col_dim]
        if component < 3:
            value = value + time_step * bulk_modulus * volume_rate
        trial_stress.append(value)
    pressure = -(trial_stress[0] + trial_stress[1] + trial_stress[2]) / 3.0
    shear_part = [trial_stress[component] + pressure for component in range(3)] + trial_stress[3:]
    shear_stress = jnp.sqrt(0.5 * (shear_part[0] ** 2 + shear_part[1] ** 2 + shear_part[2] ** 2) + shear_part[3] ** 2 + shear_part[4] ** 2 + shear_part[5] ** 2)
    shear_rate = jnp.sqrt(2.0 * (deviator[0][0] ** 2 + deviator[1][1] ** 2 + deviator[2][2] ** 2 + 2.0 * (deviator[1][2] ** 2 + deviator[0][2] ** 2 + deviator[0][1] ** 2)))
    inertial = shear_rate * grain_size / jnp.sqrt(jnp.maximum(pressure, pressure_floor) / grain_density)
    friction = friction_static + (friction_limit - friction_static) * inertial / (inertial_ref + inertial)
    support = jnp.maximum(pressure, 0.0)
    factor = jnp.minimum(1.0, friction * support / jnp.maximum(shear_stress, shear_floor))
    result = [shear_part[component] * factor - support for component in range(3)] + [shear_part[component] * factor for component in range(3, 6)]
    return jnp.stack(result)

def spline_slots(fraction, offset):
    slot_index = jnp.arange(6, dtype=jnp.int32)
    shifted = slot_index - offset[..., None]
    left_weight = 0.5 * (1.5 - fraction) ** 2
    middle = 0.75 - (fraction - 1.0) ** 2
    right_weight = 0.5 * (fraction - 0.5) ** 2
    return jnp.where(shifted == 0, left_weight[..., None], 0.0) + jnp.where(shifted == 1, middle[..., None], 0.0) + jnp.where(shifted == 2, right_weight[..., None], 0.0)

def block_weights(fraction, offset):
    along_x = spline_slots(fraction[0], offset[0])
    along_y = spline_slots(fraction[1], offset[1])
    along_z = spline_slots(fraction[2], offset[2])
    product = along_x[:, :, :, None, None] * along_y[:, :, None, :, None] * along_z[:, :, None, None, :]
    return product.reshape(product.shape[0], product.shape[1], 216)

def node_coords():
    node = jnp.arange(216, dtype=jnp.int32)
    return [(node // 36).astype(jnp.float32), (node // 6 % 6).astype(jnp.float32), (node % 6).astype(jnp.float32)]

def deposit(fraction, offset, velocity, affine, stress, live_mass):
    weights = block_weights(fraction, offset)
    position = [offset[dim_index].astype(jnp.float32) + fraction[dim_index] for dim_index in range(3)]
    matrix = [[live_mass * (affine[3 * row_dim + col_dim] - stress_scale * stress[pair_index[row_dim][col_dim]]) for col_dim in range(3)] for row_dim in range(3)]
    moment = [live_mass * velocity[row_dim] - matrix[row_dim][0] * position[0] - matrix[row_dim][1] * position[1] - matrix[row_dim][2] * position[2] for row_dim in range(3)]
    channels = jnp.stack([live_mass] + moment + [matrix[row_dim][col_dim] for row_dim in range(3) for col_dim in range(3)])
    node_sums = jnp.einsum('cgp,gpn->gcn', channels, weights, precision=lax.Precision.HIGHEST)
    coords = node_coords()
    momentum = [node_sums[:, 1 + row_dim] + node_sums[:, 4 + 3 * row_dim] * coords[0] + node_sums[:, 5 + 3 * row_dim] * coords[1] + node_sums[:, 6 + 3 * row_dim] * coords[2] for row_dim in range(3)]
    return jnp.stack(momentum + [node_sums[:, 0]], axis=1)

def collect(fraction, offset, node_values):
    weights = block_weights(fraction, offset)
    coords = node_coords()
    node_table = jnp.stack([node_values[:, row_dim] for row_dim in range(3)] + [node_values[:, row_dim] * coords[col_dim] for row_dim in range(3) for col_dim in range(3)], axis=1)
    result = jnp.einsum('gpn,gcn->cgp', weights, node_table, precision=lax.Precision.HIGHEST)
    position = [offset[dim_index].astype(jnp.float32) + fraction[dim_index] for dim_index in range(3)]
    velocity = result[0:3]
    affine = jnp.stack([4.0 * (result[3 + 3 * row_dim + col_dim] - result[row_dim] * position[col_dim]) for row_dim in range(3) for col_dim in range(3)])
    return (velocity, affine)

def grid_step(reduced, x_index, y_index, z_index, width_x, depth_z):
    inverse = 1.0 / (reduced[3] + mass_floor)
    velocity_x = reduced[0] * inverse
    velocity_y = reduced[1] * inverse - time_step * gravity
    velocity_z = reduced[2] * inverse
    outlet = (x_index >= width_x // 4) & (x_index < width_x - width_x // 4)
    floor_cells = (y_index < 2) & jnp.logical_not(outlet)
    velocity_y = jnp.where(floor_cells, jnp.maximum(velocity_y, 0.0), velocity_y)
    velocity_z = jnp.where(z_index < 2, jnp.maximum(velocity_z, 0.0), velocity_z)
    velocity_z = jnp.where(z_index >= depth_z - 2, jnp.minimum(velocity_z, 0.0), velocity_z)
    velocity_x = jnp.broadcast_to(velocity_x, velocity_y.shape)
    return jnp.stack([velocity_x, velocity_y, velocity_z])

def node_index(device, tile_ids):
    tiles_y = CY // 4
    tiles_z = CZ // 4
    corner_x = device // (N_GY * N_GZ) * CX + 4 * (tile_ids // (tiles_y * tiles_z)) - 1
    corner_y = device // N_GZ % N_GY * CY + 4 * (tile_ids // tiles_z % tiles_y) - 1
    corner_z = device % N_GZ * CZ + 4 * (tile_ids % tiles_z) - 1
    node = jnp.arange(216, dtype=jnp.int32)
    cell_x = (corner_x[:, None] + (node // 36)[None, :]) % NX
    cell_y = (corner_y[:, None] + (node // 6 % 6)[None, :]) % NY
    cell_z = (corner_z[:, None] + (node % 6)[None, :]) % NZ
    return ((cell_x * NY + cell_y) * NZ + cell_z).astype(jnp.int32)

def by_device(values):
    return jnp.moveaxis(values.reshape(values.shape[0], DEVICES, B_DEV, BLOCK), 1, 0)

def reference(point_frac, cell_offset, point_velocity, point_affine, point_stress, point_mass, block_tile, block_count):
    new_stress = stress_update(point_stress, point_affine)
    slot_index = jnp.arange(BLOCK, dtype=jnp.int32)
    live_mask = (slot_index[None, :] < block_count[:, None]).astype(jnp.float32)
    live_mass = point_mass.reshape(BLOCKS, BLOCK) * live_mask
    devices = jnp.arange(DEVICES, dtype=jnp.int32)
    frac_parts = by_device(point_frac)
    offset_parts = by_device(cell_offset)
    tile_parts = block_tile.reshape(DEVICES, B_DEV)

    def deposit_device(grid_sums, inputs):
        device, fraction, offset, velocity, affine, stress, masses, tile_ids = inputs
        node_sums = deposit(fraction, offset, velocity, affine, stress, masses)
        flat_index = node_index(device, tile_ids).reshape(-1)
        grid_sums = grid_sums.at[:, flat_index].add(jnp.moveaxis(node_sums, 1, 0).reshape(4, -1))
        return (grid_sums, None)
    grid_sums = jnp.zeros((4, NX * NY * NZ), jnp.float32)
    grid_sums, _ = lax.scan(deposit_device, grid_sums, (devices, frac_parts, offset_parts, by_device(point_velocity), by_device(point_affine), by_device(new_stress), live_mass.reshape(DEVICES, B_DEV, BLOCK), tile_parts))
    reduced = grid_sums.reshape(4, NX, NY, NZ)
    x_index = jnp.arange(NX, dtype=jnp.int32)[:, None, None]
    y_index = jnp.arange(NY, dtype=jnp.int32)[None, :, None]
    z_index = jnp.arange(NZ, dtype=jnp.int32)[None, None, :]
    grid_velocity = grid_step(reduced, x_index, y_index, z_index, NX, NZ)
    flat_velocity = grid_velocity.reshape(3, -1)

    def collect_device(carry, inputs):
        device, fraction, offset, tile_ids = inputs
        flat_index = node_index(device, tile_ids)
        node_values = jnp.moveaxis(flat_velocity[:, flat_index], 0, 1)
        velocity, affine = collect(fraction, offset, node_values)
        return (carry, (velocity, affine))
    _, outputs = lax.scan(collect_device, None, (devices, frac_parts, offset_parts, tile_parts))
    new_velocity = jnp.moveaxis(outputs[0], 0, 1).reshape(3, POINTS)
    new_affine = jnp.moveaxis(outputs[1], 0, 1).reshape(9, POINTS)
    return (new_velocity, new_affine, new_stress, grid_velocity)
```

```python
import jax
import jax.numpy as jnp
from jax import lax
from jax.experimental import pallas as pl
from jax.experimental.pallas import tpu as pltpu
from jax.sharding import PartitionSpec as P

CX = 16
CY = 64
CZ = 32
BLOCK = 128

time_step = 0.1
gravity = 1.0
shear_modulus = 2.0
bulk_modulus = 4.0
friction_static = 0.38
friction_limit = 0.64
inertial_ref = 0.28
grain_size = 0.5
grain_density = 1.0
pressure_floor = 0.5
shear_floor = 0.5
mass_floor = 0.05
stress_scale = 0.4
pair_index = ((0, 5, 4), (5, 1, 3), (4, 3, 2))
component_pairs = ((0, 0), (1, 1), (2, 2), (1, 2), (0, 2), (0, 1))

PX = CX + 2
PY = CY + 2
PZ = CZ + 2
PLANE = 4 * PZ
TILES = PX * PLANE // 8
SPAN = 5
GROUPS = -(-TILES // SPAN)
ROWS = GROUPS * SPAN * 8
REST = 2 * PY - 128
STRIDE = 40
VMEM_LIMIT = 16 * 1024 * 1024
FAR = 3.0e38


def stress_update(stress, affine):
    strain_rate = [
        [
            0.5 * (affine[3 * row_dim + col_dim] + affine[3 * col_dim + row_dim])
            for col_dim in range(3)
        ]
        for row_dim in range(3)
    ]
    volume_rate = strain_rate[0][0] + strain_rate[1][1] + strain_rate[2][2]
    deviator = [
        [
            strain_rate[row_dim][col_dim] - (volume_rate / 3.0 if row_dim == col_dim else 0.0)
            for col_dim in range(3)
        ]
        for row_dim in range(3)
    ]
    trial_stress = []
    for component in range(6):
        row_dim, col_dim = component_pairs[component]
        value = stress[component] + time_step * 2.0 * shear_modulus * deviator[row_dim][col_dim]
        if component < 3:
            value = value + time_step * bulk_modulus * volume_rate
        trial_stress.append(value)
    pressure = -(trial_stress[0] + trial_stress[1] + trial_stress[2]) / 3.0
    shear_part = [trial_stress[component] + pressure for component in range(3)] + trial_stress[3:]
    shear_stress = jnp.sqrt(
        0.5 * (shear_part[0] ** 2 + shear_part[1] ** 2 + shear_part[2] ** 2)
        + shear_part[3] ** 2
        + shear_part[4] ** 2
        + shear_part[5] ** 2
    )
    shear_rate = jnp.sqrt(
        2.0
        * (
            deviator[0][0] ** 2
            + deviator[1][1] ** 2
            + deviator[2][2] ** 2
            + 2.0 * (deviator[1][2] ** 2 + deviator[0][2] ** 2 + deviator[0][1] ** 2)
        )
    )
    inertial = (
        shear_rate * grain_size / jnp.sqrt(jnp.maximum(pressure, pressure_floor) / grain_density)
    )
    friction = friction_static + (friction_limit - friction_static) * inertial / (
        inertial_ref + inertial
    )
    support = jnp.maximum(pressure, 0.0)
    factor = jnp.minimum(1.0, friction * support / jnp.maximum(shear_stress, shear_floor))
    return [shear_part[component] * factor - support for component in range(3)] + [
        shear_part[component] * factor for component in range(3, 6)
    ]


def spline(fraction):
    left = 0.5 * (1.5 - fraction) ** 2
    middle = 0.75 - (fraction - 1.0) ** 2
    right = 0.5 * (fraction - 0.5) ** 2
    plain = (left, middle, right)
    moment = (left * (0.0 - fraction), middle * (1.0 - fraction), right * (2.0 - fraction))
    return plain, moment


def pick(masks, values):
    zero = jnp.zeros_like(values[0])
    return jnp.where(
        masks[0], values[0], jnp.where(masks[1], values[1], jnp.where(masks[2], values[2], zero))
    )


def slot_masks(slot, offset):
    shifted = slot - offset
    return (shifted == 0, shifted == 1, shifted == 2)


def x_weights(fraction, offset):
    plain, moment = spline(fraction)
    at = [offset == step for step in range(4)]
    zero = jnp.zeros_like(fraction)
    result = []
    for values in (plain, moment):
        row = []
        for slot in range(6):
            value = zero
            for node in range(3):
                if 0 <= slot - node <= 3:
                    value = jnp.where(at[slot - node], values[node], value)
            row.append(value)
        result.append(row)
    return result


def pair_weights(fraction, offset):
    plain, moment = spline(fraction)
    upper = (lax.broadcasted_iota(jnp.int32, (8, BLOCK), 0) >= 4).astype(jnp.int32)
    weight, first = [], []
    for pair in range(3):
        masks = slot_masks(upper + 2 * pair, offset)
        weight.append(pick(masks, plain))
        first.append(pick(masks, moment))
    return weight, first


def lane_weights(fraction, offset):
    plain, moment = spline(fraction)
    slot = lax.broadcasted_iota(jnp.int32, (8, BLOCK), 0)
    masks = slot_masks(slot, offset)
    return pick(masks, plain), pick(masks, moment)


def split(values):
    high = values.astype(jnp.bfloat16)
    return high, (values - high.astype(jnp.float32)).astype(jnp.bfloat16)


def point_rows(frac_ref, offset_ref, lanes):
    fraction = [jnp.broadcast_to(frac_ref[dim : dim + 1, lanes], (8, BLOCK)) for dim in range(3)]
    offset = [jnp.broadcast_to(offset_ref[dim : dim + 1, lanes], (8, BLOCK)) for dim in range(3)]
    return fraction, offset


def tile_corner(tile):
    tiles_y, tiles_z = CY // 4, CZ // 4
    tile_x = tile // (tiles_y * tiles_z)
    tile_y = (tile // tiles_z) % tiles_y
    tile_z = tile % tiles_z
    return tile_x * (4 * PLANE) + tile_z * 16, tile_y * 4


def window_rows(corner, step):
    return pl.ds(pl.multiple_of(corner + step * PLANE, 8), 24)


def lane_index():
    return lax.broadcasted_iota(jnp.int32, (8, BLOCK), 1)


def roll(values, shift):
    return pltpu.roll(values, shift % 128, 1) if shift % 128 else values


def pack_pairs(first, second, target):
    lane = lane_index()
    last = jnp.zeros((8, BLOCK), jnp.float32)
    for spot, (one, two) in enumerate(zip(first, second)):
        target[8 * spot : 8 * spot + 8, :] = jnp.where(lane < PY, one, roll(two, PY))
        last = jnp.where(lane // REST == spot, roll(two, REST * spot - (PY - REST)), last)
    target[8 * len(first) : 8 * len(first) + 8, :] = last


def unpack_pairs(source, count):
    lane = lane_index()
    last = source[8 * count : 8 * count + 8, :]
    first, second = [], []
    for spot in range(count):
        tile = source[8 * spot : 8 * spot + 8, :]
        first.append(jnp.where(lane < PY, tile, 0.0))
        tail = jnp.where(lane < PY, roll(last, (PY - REST) - REST * spot), 0.0)
        second.append(jnp.where(lane < PY - REST, roll(tile, -PY), tail))
    return first, second


def tile_rows(tile):
    return slice(8 * tile, 8 * tile + 8)


def deposit_kernel(
    blocks,
    tile_hbm,
    count_hbm,
    frac_hbm,
    offset_hbm,
    velocity_hbm,
    affine_hbm,
    stress_hbm,
    mass_hbm,
    stress_out,
    grid_ref,
    low_ref,
    high_ref,
    tile_ref,
    count_ref,
    frac_ref,
    offset_ref,
    velocity_ref,
    affine_ref,
    stress_ref,
    mass_ref,
    new_stress_ref,
    dense_ref,
    sems,
):
    sources = (
        velocity_hbm,
        affine_hbm,
        stress_hbm,
        mass_hbm,
        tile_hbm,
        count_hbm,
        frac_hbm,
        offset_hbm,
    )
    targets = (
        velocity_ref,
        affine_ref,
        stress_ref,
        mass_ref,
        tile_ref,
        count_ref,
        frac_ref,
        offset_ref,
    )
    copies = [
        pltpu.make_async_copy(source, target, sems.at[slot])
        for slot, (source, target) in enumerate(zip(sources, targets))
    ]
    for copy in copies:
        copy.start()
    grid_ref[...] = jnp.zeros_like(grid_ref)
    for copy in copies:
        copy.wait()

    def dense(component):
        return dense_ref[component * STRIDE : component * STRIDE + blocks, :]

    def put(component, values):
        dense_ref[component * STRIDE : component * STRIDE + blocks, :] = values

    for block in range(blocks):
        lanes = slice(block * BLOCK, (block + 1) * BLOCK)
        dense_ref[pl.ds(block, 3, stride=STRIDE), :] = velocity_ref[:, lanes]
        dense_ref[pl.ds(3 * STRIDE + block, 9, stride=STRIDE), :] = affine_ref[:, lanes]
        dense_ref[pl.ds(12 * STRIDE + block, 6, stride=STRIDE), :] = stress_ref[:, lanes]
    velocity = [dense(component) for component in range(3)]
    affine = [dense(3 + component) for component in range(9)]
    stress = [dense(12 + component) for component in range(6)]
    new_stress = stress_update(stress, affine)
    for component in range(6):
        put(12 + component, new_stress[component])
    mass = mass_ref[...]
    columns = [[mass * velocity[row] for row in range(3)] + [mass]]
    for col in range(3):
        columns.append(
            [
                mass * (affine[3 * row + col] - stress_scale * new_stress[pair_index[row][col]])
                for row in range(3)
            ]
            + [jnp.zeros_like(mass)]
        )
    for group in range(4):
        for channel in range(4):
            put(18 + 8 * group + channel, columns[group][channel])
            put(18 + 8 * group + 4 + channel, columns[group][channel])
    for block in range(blocks):
        lanes = slice(block * BLOCK, (block + 1) * BLOCK)
        new_stress_ref[:, lanes] = dense_ref[pl.ds(12 * STRIDE + block, 6, stride=STRIDE), :]
    stress_copy = pltpu.make_async_copy(new_stress_ref, stress_out, sems.at[len(copies)])
    stress_copy.start()

    lane = lane_index()

    def one_block(block, carry):
        lanes = pl.ds(pl.multiple_of(block * BLOCK, BLOCK), BLOCK)
        corner, corner_y = tile_corner(tile_ref[block])
        fraction, offset = point_rows(frac_ref, offset_ref, lanes)
        base, col_x, col_y, col_z = [
            dense_ref[pl.ds((18 + 8 * group) * STRIDE + block, 8, stride=STRIDE), :]
            for group in range(4)
        ]
        weight_x, first_x = x_weights(fraction[0], offset[0])
        weight_z, first_z = pair_weights(fraction[2], offset[2])
        offset_y = jnp.where(lane < count_ref[block], offset[1], -100)
        weight_y, first_y = lane_weights(fraction[1], offset_y)
        right = jnp.concatenate([weight_y, first_y], axis=1)
        flat = [base * weight_z[pair] + col_z * first_z[pair] for pair in range(3)]
        along = [col_x * weight_z[pair] for pair in range(3)]
        depth = [col_y * weight_z[pair] for pair in range(3)]
        left = jnp.concatenate(
            [
                jnp.concatenate(
                    [
                        weight_x[step] * flat[pair] + first_x[step] * along[pair]
                        for step in range(6)
                        for pair in range(3)
                    ],
                    axis=0,
                ),
                jnp.concatenate(
                    [weight_x[step] * depth[pair] for step in range(6) for pair in range(3)],
                    axis=0,
                ),
            ],
            axis=1,
        )
        left_high, left_low = split(left)
        fill = jnp.zeros((BLOCK - 8, 2 * BLOCK), jnp.float32)
        right_high, right_low = split(jnp.concatenate([right, fill], axis=0))

        def dot(one, two):
            return lax.dot_general(
                one, two, (((1,), (1,)), ((), ())), preferred_element_type=jnp.float32
            )

        sums = dot(left_high, right_high) + dot(left_low, right_high) + dot(left_high, right_low)
        for step in range(6):
            rows = window_rows(corner, step)
            grid_ref[rows, :] += pltpu.roll(sums[24 * step : 24 * step + 24], corner_y, 1)
        return carry

    lax.fori_loop(0, blocks, one_block, 0, unroll=4)

    low = [jnp.zeros((8, BLOCK), jnp.float32) for _ in range(SPAN)]
    high = [jnp.zeros((8, BLOCK), jnp.float32) for _ in range(SPAN)]
    for group in range(GROUPS):
        low_mask = lane // 2 == group
        high_mask = lane // 2 == (CY // 2 + group) % 64
        for spot in range(SPAN):
            tile = group * SPAN + spot
            if tile < TILES:
                turned = roll(grid_ref[tile_rows(tile), :], 2 * group)
                low[spot] = jnp.where(low_mask, turned, low[spot])
                high[spot] = jnp.where(high_mask, turned, high[spot])
    for spot in range(SPAN):
        low_ref[tile_rows(spot), :] = low[spot]
        high_ref[tile_rows(spot), :] = high[spot]
    stress_copy.wait()


def add_y(grid_ref, above, below, tiles):
    lane = lane_index()
    bottom, top = lane // 2 == 0, lane // 2 == CY // 2
    for tile in tiles:
        group, spot = divmod(tile, SPAN)
        lower = roll(below[spot], -CY - 2 * group)
        upper = roll(above[spot], CY - 2 * group)
        grid_ref[tile_rows(tile), :] += jnp.where(bottom, lower, jnp.where(top, upper, 0.0))


FACE = PLANE // 8


def join_y_faces(above_ref, below_ref, _, grid_ref, low_ref, high_ref):
    above = [above_ref[tile_rows(spot), :] for spot in range(SPAN)]
    below = [below_ref[tile_rows(spot), :] for spot in range(SPAN)]
    tiles = [step * FACE + side for step in range(PX) for side in (0, FACE - 1)]
    add_y(grid_ref, above, below, tiles)
    half = PX // 2
    for target, side in ((low_ref, 0), (high_ref, FACE - 1)):
        faces = [grid_ref[tile_rows(step * FACE + side), :] for step in range(PX)]
        pack_pairs(faces[:half], faces[half:], target)


def join_y_rest(above_ref, below_ref, _, grid_ref):
    above = [above_ref[tile_rows(spot), :] for spot in range(SPAN)]
    below = [below_ref[tile_rows(spot), :] for spot in range(SPAN)]
    tiles = [step * FACE + side for step in range(PX) for side in range(1, FACE - 1)]
    add_y(grid_ref, above, below, tiles)


def join_z(above_ref, below_ref, _, grid_ref, low_ref, high_ref):
    half = PX // 2
    for source, side in ((below_ref, 0), (above_ref, FACE - 1)):
        first, second = unpack_pairs(source, half)
        for step, value in enumerate(first + second):
            grid_ref[tile_rows(step * FACE + side), :] += value
    for target, start in ((low_ref, 0), (high_ref, CX)):
        planes = [
            [grid_ref[tile_rows((start + part) * FACE + spot), :] for spot in range(FACE)]
            for part in range(2)
        ]
        pack_pairs(planes[0], planes[1], target)


def place_bounds(place_ref):
    place = [place_ref[axis] for axis in range(3)]
    width = [place_ref[3 + axis] for axis in range(3)]
    at_y = lax.rem(place[1] * CY + lane_index() - 1 + width[1], width[1])
    return place, width, at_y < 2


def floor_of(at_x, width_x, low_y):
    outlet = (at_x >= width_x // 4) & (at_x < width_x - width_x // 4)
    return jnp.where(low_y & jnp.logical_not(outlet), 0.0, -FAR)


def bounds_z(at_z, depth_z):
    return jnp.where(at_z < 2, 0.0, -FAR), jnp.where(at_z >= depth_z - 2, 0.0, FAR)


def velocities(parts, floor, bounds):
    inverse = 1.0 / (parts[3] + mass_floor)
    u_x = parts[0] * inverse
    u_y = jnp.maximum(parts[1] * inverse - time_step * gravity, floor)
    u_z = parts[2] * inverse
    if bounds is not None:
        u_z = jnp.minimum(jnp.maximum(u_z, bounds[0]), bounds[1])
    return u_x, u_y, u_z


def settle_plane(place_ref, source_ref, source_row, u_ref, step, out_ref, out_step):
    place, width, low_y = place_bounds(place_ref)
    sublane = lax.broadcasted_iota(jnp.int32, (8, BLOCK), 0)
    at_x = lax.rem(place[0] * CX + step - 1 + width[0], width[0])
    floor = floor_of(at_x, width[0], low_y)
    for group in range(CZ // 8):
        start = 4 + 32 * group
        parts = [
            source_ref[pl.ds(source_row + start + channel, 8, stride=4), :] for channel in range(4)
        ]
        bounds = None
        if group in (0, CZ // 8 - 1):
            bounds = bounds_z(place[2] * CZ + 8 * group + sublane, width[2])
        values = velocities(parts, floor, bounds)
        for channel in range(3):
            u_ref[pl.ds(step * PLANE + start + channel, 8, stride=4), :] = values[channel]
            if out_step is not None:
                out_ref[channel, out_step, 8 * group : 8 * group + 8, :] = roll(
                    values[channel], -1
                )[:, 0:CY]


def settle_edges(place_ref, source_ref, source_row, u_ref, first, count):
    place, width, low_y = place_bounds(place_ref)
    sublane = lax.broadcasted_iota(jnp.int32, (8, BLOCK), 0)
    at_x = lax.rem(place[0] * CX + first + sublane - 1 + width[0], width[0])
    floor = floor_of(at_x, width[0], low_y)
    for edge in (0, CZ + 1):
        at_z = lax.rem(place[2] * CZ + edge - 1 + width[2], width[2])
        bounds = bounds_z(at_z + 0 * sublane, width[2])
        parts = [
            source_ref[pl.ds(source_row + 4 * edge + channel, count, stride=PLANE), :]
            for channel in range(4)
        ]
        values = velocities(parts, floor[0:count], [bound[0:count] for bound in bounds])
        for channel in range(3):
            start = first * PLANE + 4 * edge + channel
            u_ref[pl.ds(start, count, stride=PLANE), :] = values[channel]


def settle_kernel(place_ref, grid_ref, u_ref, out_hbm, out_ref, sem):
    def plane(step, carry):
        row = pl.multiple_of(step * PLANE, 8)
        settle_plane(place_ref, grid_ref, row, u_ref, step, out_ref, step - 2)
        return carry

    lax.fori_loop(2, CX, plane, 0, unroll=2)
    copy = pltpu.make_async_copy(out_ref, out_hbm.at[:, pl.ds(1, CX - 2)], sem)
    copy.start()
    for first in range(2, CX, 8):
        count = min(8, CX - first)
        settle_edges(place_ref, grid_ref, first * PLANE, u_ref, first, count)
    copy.wait()


def collect_kernel(
    blocks,
    place_ref,
    tile_ref,
    above_ref,
    below_ref,
    frac_ref,
    offset_ref,
    grid_ref,
    _,
    __,
    u_ref,
    out_hbm,
    velocity_hbm,
    affine_hbm,
    edge_ref,
    out_ref,
    stage_ref,
    velocity_ref,
    affine_ref,
    sems,
):
    for source, start, spot in ((below_ref, 0, 0), (above_ref, CX, 2)):
        first, second = unpack_pairs(source, FACE)
        for tile, value in enumerate(first + second):
            edge_ref[tile_rows(spot * FACE + tile), :] = (
                grid_ref[tile_rows(start * FACE + tile), :] + value
            )
    for spot, step in enumerate((0, 1, CX, CX + 1)):
        out_step = {1: 0, CX: 1}.get(step)
        settle_plane(place_ref, edge_ref, spot * PLANE, u_ref, step, out_ref, out_step)
    settle_edges(place_ref, edge_ref, 0, u_ref, 0, 2)
    settle_edges(place_ref, edge_ref, 2 * PLANE, u_ref, CX, 2)
    copies = [
        pltpu.make_async_copy(
            out_ref.at[:, pl.ds(slot, 1)],
            out_hbm.at[:, pl.ds(slot * (CX - 1), 1)],
            sems.at[slot],
        )
        for slot in range(2)
    ]
    for copy in copies:
        copy.start()
    lane = lane_index()

    def one_block(block, carry):
        lanes = pl.ds(pl.multiple_of(block * BLOCK, BLOCK), BLOCK)
        corner, corner_y = tile_corner(tile_ref[block])
        fraction, offset = point_rows(frac_ref, offset_ref, lanes)
        weight_x, first_x = x_weights(fraction[0], offset[0])
        weight_z, first_z = pair_weights(fraction[2], offset[2])
        weight_y, first_y = lane_weights(fraction[1], offset[1])
        right_high, right_low = split(jnp.concatenate([weight_y, first_y], axis=1))
        right = jnp.concatenate(
            [
                right_high.astype(jnp.float32),
                right_high.astype(jnp.float32),
                right_low.astype(jnp.float32),
                jnp.zeros((BLOCK - 24, 2 * BLOCK), jnp.float32),
            ],
            axis=0,
        ).astype(jnp.bfloat16)
        nodes = jnp.concatenate(
            [
                pltpu.roll(u_ref[window_rows(corner, step), :], (128 - corner_y) & 127, 1)
                for step in range(6)
            ],
            axis=0,
        )
        high = nodes.astype(jnp.bfloat16).astype(jnp.float32)
        low = nodes - high
        at = lax.broadcasted_iota(jnp.int32, nodes.shape, 1)
        left = jnp.where(
            at < 8, high, jnp.where(at < 16, pltpu.roll(low, 8, 1), pltpu.roll(high, 16, 1))
        ).astype(jnp.bfloat16)
        sums = lax.dot_general(
            left, right, (((1,), (0,)), ((), ())), preferred_element_type=jnp.float32
        )

        def over_x(weights, column):
            result = []
            for pair in range(3):
                total = None
                for step in range(6):
                    row = 24 * step + 8 * pair
                    term = weights[step] * sums[row : row + 8, column : column + BLOCK]
                    total = term if total is None else total + term
                result.append(total)
            return result

        def over_z(weights, values):
            total = weights[0] * values[0] + weights[1] * values[1] + weights[2] * values[2]
            return total + pltpu.roll(total, 4, 0)

        plain = over_x(weight_x, 0)
        velocity = over_z(weight_z, plain)
        columns = (
            over_z(weight_z, over_x(first_x, 0)),
            over_z(weight_z, over_x(weight_x, BLOCK)),
            over_z(first_z, plain),
        )
        velocity_ref[:, lanes] = velocity[0:3]
        for col in range(3):
            stage_ref[pl.ds(block * 16 + col, 3, stride=3), :] = 4.0 * columns[col][0:3]
        affine_ref[:, lanes] = stage_ref[pl.ds(pl.multiple_of(block * 16, 8), 9), :]
        return carry

    del lane
    lax.fori_loop(0, blocks, one_block, 0, unroll=4)
    last = [
        pltpu.make_async_copy(velocity_ref, velocity_hbm, sems.at[2]),
        pltpu.make_async_copy(affine_ref, affine_hbm, sems.at[3]),
    ]
    for copy in last:
        copy.start()
    for copy in copies + last:
        copy.wait()


def exchange(low, high, axis):
    count = lax.axis_size(axis)
    up = [(i, (i + 1) % count) for i in range(count)]
    down = [(target, source) for source, target in up]
    return lax.ppermute(low, axis, down), lax.ppermute(high, axis, up)


def shards(
    point_frac,
    cell_offset,
    point_velocity,
    point_affine,
    point_stress,
    point_mass,
    block_tile,
    block_count,
):
    blocks = block_tile.shape[0]
    points = blocks * BLOCK
    f32 = jnp.float32
    vmem = pl.BlockSpec(memory_space=pltpu.VMEM)
    smem = pl.BlockSpec(memory_space=pltpu.SMEM)
    hbm = pl.BlockSpec(memory_space=pltpu.HBM)
    params = pltpu.CompilerParams(vmem_limit_bytes=VMEM_LIMIT)
    grid_shape = jax.ShapeDtypeStruct((ROWS, BLOCK), f32)
    out_shape = jax.ShapeDtypeStruct((3, CX, CZ, CY), f32)

    def message(tiles):
        return jax.ShapeDtypeStruct((8 * tiles, BLOCK), f32)

    def cost(microseconds):
        return pl.CostEstimate(
            flops=int(microseconds * 8.0e6), bytes_accessed=1000, transcendentals=0
        )

    mass = point_mass.reshape(blocks, BLOCK)
    inputs = (
        block_tile,
        block_count,
        point_frac,
        cell_offset,
        point_velocity,
        point_affine,
        point_stress,
        mass,
    )
    new_stress, grid, low, high = pl.pallas_call(
        lambda *refs: deposit_kernel(blocks, *refs),
        out_shape=(
            jax.ShapeDtypeStruct((6, points), f32),
            grid_shape,
            message(SPAN),
            message(SPAN),
        ),
        in_specs=[hbm] * 8,
        out_specs=(hbm, vmem, vmem, vmem),
        scratch_shapes=[
            pltpu.SMEM(block_tile.shape, jnp.int32),
            pltpu.SMEM(block_count.shape, jnp.int32),
        ]
        + [pltpu.VMEM(array.shape, array.dtype) for array in inputs[2:]]
        + [
            pltpu.VMEM((6, points), f32),
            pltpu.VMEM((50 * STRIDE, BLOCK), f32),
            pltpu.SemaphoreType.DMA((9,)),
        ],
        compiler_params=params,
        cost_estimate=cost(5),
        name="deposit",
    )(*[pltpu.with_memory_space_constraint(array, pltpu.HBM) for array in inputs])
    above, below = exchange(low, high, "gy")
    grid, low, high = pl.pallas_call(
        join_y_faces,
        out_shape=(grid_shape, message(PX // 2 + 1), message(PX // 2 + 1)),
        in_specs=[vmem] * 3,
        out_specs=(vmem,) * 3,
        input_output_aliases={2: 0},
        compiler_params=params,
        cost_estimate=cost(0.3),
        name="join_y_faces",
    )(above, below, grid)
    grid = pl.pallas_call(
        join_y_rest,
        out_shape=grid_shape,
        in_specs=[vmem] * 3,
        out_specs=vmem,
        input_output_aliases={2: 0},
        compiler_params=params,
        cost_estimate=cost(1),
        name="join_y_rest",
    )(above, below, grid)
    above, below = exchange(low, high, "gz")
    grid, low, high = pl.pallas_call(
        join_z,
        out_shape=(grid_shape, message(FACE + 1), message(FACE + 1)),
        in_specs=[vmem] * 3,
        out_specs=(vmem,) * 3,
        input_output_aliases={2: 0},
        compiler_params=params,
        cost_estimate=cost(0.3),
        name="join_z",
    )(above, below, grid)
    above, below = exchange(low, high, "gx")
    place = jnp.stack(
        [lax.axis_index("gx"), lax.axis_index("gy"), lax.axis_index("gz")]
        + [
            jnp.int32(lax.axis_size("gx") * CX),
            jnp.int32(lax.axis_size("gy") * CY),
            jnp.int32(lax.axis_size("gz") * CZ),
        ]
    )
    speed, grid_velocity = pl.pallas_call(
        settle_kernel,
        out_shape=(grid_shape, out_shape),
        in_specs=[smem, vmem],
        out_specs=(vmem, hbm),
        scratch_shapes=[pltpu.VMEM((3, CX - 2, CZ, CY), f32), pltpu.SemaphoreType.DMA],
        compiler_params=params,
        cost_estimate=cost(2),
        name="settle",
    )(place, grid)
    _, grid_velocity, new_velocity, new_affine = pl.pallas_call(
        lambda *refs: collect_kernel(blocks, *refs),
        out_shape=(
            grid_shape,
            out_shape,
            jax.ShapeDtypeStruct((3, points), f32),
            jax.ShapeDtypeStruct((9, points), f32),
        ),
        in_specs=[smem, smem] + [vmem] * 6 + [hbm],
        out_specs=(vmem, hbm, hbm, hbm),
        input_output_aliases={7: 0, 8: 1},
        scratch_shapes=[
            pltpu.VMEM((4 * PLANE, BLOCK), f32),
            pltpu.VMEM((3, 2, CZ, CY), f32),
            pltpu.VMEM((blocks * 16, BLOCK), f32),
            pltpu.VMEM((3, points), f32),
            pltpu.VMEM((9, points), f32),
            pltpu.SemaphoreType.DMA((4,)),
        ],
        compiler_params=params,
        cost_estimate=cost(4),
        name="collect",
    )(place, block_tile, above, below, point_frac, cell_offset, grid, speed, grid_velocity)
    return (new_velocity, new_affine, new_stress, grid_velocity.transpose(0, 1, 3, 2))


def solution(mesh):
    points = ("gx", "gy", "gz")
    return jax.shard_map(
        shards,
        mesh=mesh,
        in_specs=(P(None, points),) * 5 + (P(points),) * 3,
        out_specs=(P(None, points),) * 3 + (P(None, "gx", "gy", "gz"),),
        check_vma=False,
    )
```

```python
import jax
import jax.numpy as jnp
from jax import lax
from jax.experimental import pallas as pl
from jax.experimental.pallas import tpu as pltpu
from jax.sharding import PartitionSpec as P

CX = 16
CY = 64
CZ = 32
BLOCK = 128

time_step = 0.1
gravity = 1.0
shear_modulus = 2.0
bulk_modulus = 4.0
friction_static = 0.38
friction_limit = 0.64
inertial_ref = 0.28
grain_size = 0.5
grain_density = 1.0
pressure_floor = 0.5
shear_floor = 0.5
mass_floor = 0.05
stress_scale = 0.4
pair_index = ((0, 5, 4), (5, 1, 3), (4, 3, 2))
component_pairs = ((0, 0), (1, 1), (2, 2), (1, 2), (0, 2), (0, 1))

PX = CX + 2
PY = CY + 2
PZ = CZ + 2
PLANE = 4 * PZ
TILES = PX * PLANE // 8
SPAN = 5
GROUPS = -(-TILES // SPAN)
ROWS = GROUPS * SPAN * 8
REST = 2 * PY - 128
STRIDE = 40
CHUNK = 16
VMEM_LIMIT = 16 * 1024 * 1024
FAR = 3.0e38


def stress_update(stress, affine):
    strain_rate = [
        [
            0.5 * (affine[3 * row_dim + col_dim] + affine[3 * col_dim + row_dim])
            for col_dim in range(3)
        ]
        for row_dim in range(3)
    ]
    volume_rate = strain_rate[0][0] + strain_rate[1][1] + strain_rate[2][2]
    deviator = [
        [
            strain_rate[row_dim][col_dim] - (volume_rate / 3.0 if row_dim == col_dim else 0.0)
            for col_dim in range(3)
        ]
        for row_dim in range(3)
    ]
    trial_stress = []
    for component in range(6):
        row_dim, col_dim = component_pairs[component]
        value = stress[component] + time_step * 2.0 * shear_modulus * deviator[row_dim][col_dim]
        if component < 3:
            value = value + time_step * bulk_modulus * volume_rate
        trial_stress.append(value)
    pressure = -(trial_stress[0] + trial_stress[1] + trial_stress[2]) / 3.0
    shear_part = [trial_stress[component] + pressure for component in range(3)] + trial_stress[3:]
    shear_stress = jnp.sqrt(
        0.5 * (shear_part[0] ** 2 + shear_part[1] ** 2 + shear_part[2] ** 2)
        + shear_part[3] ** 2
        + shear_part[4] ** 2
        + shear_part[5] ** 2
    )
    shear_rate = jnp.sqrt(
        2.0
        * (
            deviator[0][0] ** 2
            + deviator[1][1] ** 2
            + deviator[2][2] ** 2
            + 2.0 * (deviator[1][2] ** 2 + deviator[0][2] ** 2 + deviator[0][1] ** 2)
        )
    )
    inertial = (
        shear_rate * grain_size / jnp.sqrt(jnp.maximum(pressure, pressure_floor) / grain_density)
    )
    friction = friction_static + (friction_limit - friction_static) * inertial / (
        inertial_ref + inertial
    )
    support = jnp.maximum(pressure, 0.0)
    factor = jnp.minimum(1.0, friction * support / jnp.maximum(shear_stress, shear_floor))
    return [shear_part[component] * factor - support for component in range(3)] + [
        shear_part[component] * factor for component in range(3, 6)
    ]


def spline(fraction):
    left = 0.5 * (1.5 - fraction) ** 2
    middle = 0.75 - (fraction - 1.0) ** 2
    right = 0.5 * (fraction - 0.5) ** 2
    plain = (left, middle, right)
    moment = (left * (0.0 - fraction), middle * (1.0 - fraction), right * (2.0 - fraction))
    return plain, moment


def pick(masks, values):
    zero = jnp.zeros_like(values[0])
    return jnp.where(
        masks[0], values[0], jnp.where(masks[1], values[1], jnp.where(masks[2], values[2], zero))
    )


def slot_masks(slot, offset):
    shifted = slot - offset
    return (shifted == 0, shifted == 1, shifted == 2)


def x_weights(fraction, offset):
    plain, moment = spline(fraction)
    at = [offset == step for step in range(4)]
    zero = jnp.zeros_like(fraction)
    result = []
    for values in (plain, moment):
        row = []
        for slot in range(6):
            value = zero
            for node in range(3):
                if 0 <= slot - node <= 3:
                    value = jnp.where(at[slot - node], values[node], value)
            row.append(value)
        result.append(row)
    return result


def pair_weights(fraction, offset):
    plain, moment = spline(fraction)
    upper = (lax.broadcasted_iota(jnp.int32, (8, BLOCK), 0) >= 4).astype(jnp.int32)
    weight, first = [], []
    for pair in range(3):
        masks = slot_masks(upper + 2 * pair, offset)
        weight.append(pick(masks, plain))
        first.append(pick(masks, moment))
    return weight, first


def lane_weights(fraction, offset):
    plain, moment = spline(fraction)
    slot = lax.broadcasted_iota(jnp.int32, (8, BLOCK), 0)
    masks = slot_masks(slot, offset)
    return pick(masks, plain), pick(masks, moment)


def split(values):
    high = values.astype(jnp.bfloat16)
    return high, (values - high.astype(jnp.float32)).astype(jnp.bfloat16)


def point_rows(frac_ref, offset_ref, lanes):
    fraction = [jnp.broadcast_to(frac_ref[dim : dim + 1, lanes], (8, BLOCK)) for dim in range(3)]
    offset = [jnp.broadcast_to(offset_ref[dim : dim + 1, lanes], (8, BLOCK)) for dim in range(3)]
    return fraction, offset


def tile_corner(tile):
    tiles_y, tiles_z = CY // 4, CZ // 4
    tile_x = tile // (tiles_y * tiles_z)
    tile_y = (tile // tiles_z) % tiles_y
    tile_z = tile % tiles_z
    return tile_x * (4 * PLANE) + tile_z * 16, tile_y * 4


def expansion():
    row = lax.broadcasted_iota(jnp.int32, (2 * BLOCK, 2 * BLOCK), 0)
    col = lax.broadcasted_iota(jnp.int32, (2 * BLOCK, 2 * BLOCK), 1)
    source = (col // 16) * 4 + col % 8 + jnp.where(col % 16 < 8, 0, BLOCK)
    return jnp.where(row == source, 1.0, 0.0).astype(jnp.bfloat16)


def expand(values, matrix, spread_ref, row):
    wide = jnp.dot(
        jnp.concatenate(split(values), axis=1), matrix, preferred_element_type=jnp.float32
    )
    count = values.shape[0]
    spread_ref[pl.ds(pl.multiple_of(row, 8), count), :] = wide[:, 0:BLOCK]
    spread_ref[pl.ds(pl.multiple_of(row + PX * PLANE, 8), count), :] = wide[:, BLOCK:]


def window_rows(corner, step):
    return pl.ds(pl.multiple_of(corner + step * PLANE, 8), 24)


def lane_index():
    return lax.broadcasted_iota(jnp.int32, (8, BLOCK), 1)


def roll(values, shift):
    return pltpu.roll(values, shift % 128, 1) if shift % 128 else values


def pack_pairs(first, second, target):
    lane = lane_index()
    last = jnp.zeros((8, BLOCK), jnp.float32)
    for spot, (one, two) in enumerate(zip(first, second)):
        target[8 * spot : 8 * spot + 8, :] = jnp.where(lane < PY, one, roll(two, PY))
        last = jnp.where(lane // REST == spot, roll(two, REST * spot - (PY - REST)), last)
    target[8 * len(first) : 8 * len(first) + 8, :] = last


def unpack_pairs(source, count):
    lane = lane_index()
    last = source[8 * count : 8 * count + 8, :]
    first, second = [], []
    for spot in range(count):
        tile = source[8 * spot : 8 * spot + 8, :]
        first.append(jnp.where(lane < PY, tile, 0.0))
        tail = jnp.where(lane < PY, roll(last, (PY - REST) - REST * spot), 0.0)
        second.append(jnp.where(lane < PY - REST, roll(tile, -PY), tail))
    return first, second


def tile_rows(tile):
    return slice(8 * tile, 8 * tile + 8)


def deposit_kernel(
    blocks,
    tile_hbm,
    count_hbm,
    frac_hbm,
    offset_hbm,
    velocity_hbm,
    affine_hbm,
    stress_hbm,
    mass_hbm,
    stress_out,
    grid_ref,
    low_ref,
    high_ref,
    tile_ref,
    count_ref,
    frac_ref,
    offset_ref,
    velocity_ref,
    affine_ref,
    stress_ref,
    mass_ref,
    new_stress_ref,
    dense_ref,
    sems,
):
    sources = (
        velocity_hbm,
        affine_hbm,
        stress_hbm,
        mass_hbm,
        tile_hbm,
        count_hbm,
        frac_hbm,
        offset_hbm,
    )
    targets = (
        velocity_ref,
        affine_ref,
        stress_ref,
        mass_ref,
        tile_ref,
        count_ref,
        frac_ref,
        offset_ref,
    )
    copies = [
        pltpu.make_async_copy(source, target, sems.at[slot])
        for slot, (source, target) in enumerate(zip(sources, targets))
    ]
    for copy in copies:
        copy.start()
    grid_ref[...] = jnp.zeros_like(grid_ref)
    for copy in copies:
        copy.wait()

    def dense(component):
        return dense_ref[component * STRIDE : component * STRIDE + blocks, :]

    def put(component, values):
        dense_ref[component * STRIDE : component * STRIDE + blocks, :] = values

    for block in range(blocks):
        lanes = slice(block * BLOCK, (block + 1) * BLOCK)
        dense_ref[pl.ds(block, 3, stride=STRIDE), :] = velocity_ref[:, lanes]
        dense_ref[pl.ds(3 * STRIDE + block, 9, stride=STRIDE), :] = affine_ref[:, lanes]
        dense_ref[pl.ds(12 * STRIDE + block, 6, stride=STRIDE), :] = stress_ref[:, lanes]
    velocity = [dense(component) for component in range(3)]
    affine = [dense(3 + component) for component in range(9)]
    stress = [dense(12 + component) for component in range(6)]
    new_stress = stress_update(stress, affine)
    for component in range(6):
        put(12 + component, new_stress[component])
    mass = mass_ref[...]
    columns = [[mass * velocity[row] for row in range(3)] + [mass]]
    for col in range(3):
        columns.append(
            [
                mass * (affine[3 * row + col] - stress_scale * new_stress[pair_index[row][col]])
                for row in range(3)
            ]
            + [jnp.zeros_like(mass)]
        )
    for group in range(4):
        for channel in range(4):
            put(18 + 8 * group + channel, columns[group][channel])
            put(18 + 8 * group + 4 + channel, columns[group][channel])
    for block in range(blocks):
        lanes = slice(block * BLOCK, (block + 1) * BLOCK)
        new_stress_ref[:, lanes] = dense_ref[pl.ds(12 * STRIDE + block, 6, stride=STRIDE), :]
    stress_copy = pltpu.make_async_copy(new_stress_ref, stress_out, sems.at[len(copies)])
    stress_copy.start()

    lane = lane_index()

    def one_block(block, carry):
        lanes = pl.ds(pl.multiple_of(block * BLOCK, BLOCK), BLOCK)
        corner, corner_y = tile_corner(tile_ref[block])
        fraction, offset = point_rows(frac_ref, offset_ref, lanes)
        base, col_x, col_y, col_z = [
            dense_ref[pl.ds((18 + 8 * group) * STRIDE + block, 8, stride=STRIDE), :]
            for group in range(4)
        ]
        weight_x, first_x = x_weights(fraction[0], offset[0])
        weight_z, first_z = pair_weights(fraction[2], offset[2])
        offset_y = jnp.where(lane < count_ref[block], offset[1], -100)
        weight_y, first_y = lane_weights(fraction[1], offset_y)
        right = jnp.concatenate([weight_y, first_y], axis=1)
        flat = [base * weight_z[pair] + col_z * first_z[pair] for pair in range(3)]
        along = [col_x * weight_z[pair] for pair in range(3)]
        depth = [col_y * weight_z[pair] for pair in range(3)]
        left = jnp.concatenate(
            [
                jnp.concatenate(
                    [
                        weight_x[step] * flat[pair] + first_x[step] * along[pair]
                        for step in range(6)
                        for pair in range(3)
                    ],
                    axis=0,
                ),
                jnp.concatenate(
                    [weight_x[step] * depth[pair] for step in range(6) for pair in range(3)],
                    axis=0,
                ),
            ],
            axis=1,
        )
        left_high, left_low = split(left)
        fill = jnp.zeros((BLOCK - 8, 2 * BLOCK), jnp.float32)
        right_high, right_low = split(jnp.concatenate([right, fill], axis=0))

        def dot(one, two):
            return lax.dot_general(
                one, two, (((1,), (1,)), ((), ())), preferred_element_type=jnp.float32
            )

        sums = dot(left_high, right_high) + dot(left_low, right_high) + dot(left_high, right_low)
        for step in range(6):
            rows = window_rows(corner, step)
            grid_ref[rows, :] += pltpu.roll(sums[24 * step : 24 * step + 24], corner_y, 1)
        return carry

    lax.fori_loop(0, blocks, one_block, 0, unroll=min(blocks, 32))

    low = [jnp.zeros((8, BLOCK), jnp.float32) for _ in range(SPAN)]
    high = [jnp.zeros((8, BLOCK), jnp.float32) for _ in range(SPAN)]
    for group in range(GROUPS):
        low_mask = lane // 2 == group
        high_mask = lane // 2 == (CY // 2 + group) % 64
        for spot in range(SPAN):
            tile = group * SPAN + spot
            if tile < TILES:
                turned = roll(grid_ref[tile_rows(tile), :], 2 * group)
                low[spot] = jnp.where(low_mask, turned, low[spot])
                high[spot] = jnp.where(high_mask, turned, high[spot])
    for spot in range(SPAN):
        low_ref[tile_rows(spot), :] = low[spot]
        high_ref[tile_rows(spot), :] = high[spot]
    stress_copy.wait()


def add_y(grid_ref, above, below, tiles):
    lane = lane_index()
    bottom, top = lane // 2 == 0, lane // 2 == CY // 2
    for tile in tiles:
        group, spot = divmod(tile, SPAN)
        lower = roll(below[spot], -CY - 2 * group)
        upper = roll(above[spot], CY - 2 * group)
        grid_ref[tile_rows(tile), :] += jnp.where(bottom, lower, jnp.where(top, upper, 0.0))


FACE = PLANE // 8


def join_y_faces(above_ref, below_ref, _, grid_ref, low_ref, high_ref):
    above = [above_ref[tile_rows(spot), :] for spot in range(SPAN)]
    below = [below_ref[tile_rows(spot), :] for spot in range(SPAN)]
    tiles = [step * FACE + side for step in range(PX) for side in (0, FACE - 1)]
    add_y(grid_ref, above, below, tiles)
    half = PX // 2
    for target, side in ((low_ref, 0), (high_ref, FACE - 1)):
        faces = [grid_ref[tile_rows(step * FACE + side), :] for step in range(PX)]
        pack_pairs(faces[:half], faces[half:], target)


def join_y_rest(above_ref, below_ref, _, grid_ref):
    above = [above_ref[tile_rows(spot), :] for spot in range(SPAN)]
    below = [below_ref[tile_rows(spot), :] for spot in range(SPAN)]
    tiles = [step * FACE + side for step in range(PX) for side in range(1, FACE - 1)]
    add_y(grid_ref, above, below, tiles)


def join_z(above_ref, below_ref, _, grid_ref, low_ref, high_ref):
    half = PX // 2
    for source, side in ((below_ref, 0), (above_ref, FACE - 1)):
        first, second = unpack_pairs(source, half)
        for step, value in enumerate(first + second):
            grid_ref[tile_rows(step * FACE + side), :] += value
    for target, start in ((low_ref, 0), (high_ref, CX)):
        planes = [
            [grid_ref[tile_rows((start + part) * FACE + spot), :] for spot in range(FACE)]
            for part in range(2)
        ]
        pack_pairs(planes[0], planes[1], target)


def place_bounds():
    axes = ("gx", "gy", "gz")
    place = [lax.axis_index(axis) for axis in axes]
    width = [lax.axis_size(axis) * cells for axis, cells in zip(axes, (CX, CY, CZ))]
    at_y = lax.rem(place[1] * CY + lane_index() - 1 + width[1], width[1])
    return place, width, at_y < 2


def floor_of(at_x, width_x, low_y):
    outlet = (at_x >= width_x // 4) & (at_x < width_x - width_x // 4)
    return jnp.where(low_y & jnp.logical_not(outlet), 0.0, -FAR)


def bounds_z(at_z, depth_z):
    return jnp.where(at_z < 2, 0.0, -FAR), jnp.where(at_z >= depth_z - 2, 0.0, FAR)


def velocities(parts, floor, bounds):
    inverse = 1.0 / (parts[3] + mass_floor)
    u_x = parts[0] * inverse
    u_y = jnp.maximum(parts[1] * inverse - time_step * gravity, floor)
    u_z = parts[2] * inverse
    if bounds is not None:
        u_z = jnp.minimum(jnp.maximum(u_z, bounds[0]), bounds[1])
    return u_x, u_y, u_z


def settle_plane(source_ref, source_row, u_ref, step, out_ref, out_step, spot=None):
    spot = step if spot is None else spot
    place, width, low_y = place_bounds()
    sublane = lax.broadcasted_iota(jnp.int32, (8, BLOCK), 0)
    at_x = lax.rem(place[0] * CX + step - 1 + width[0], width[0])
    floor = floor_of(at_x, width[0], low_y)
    for group in range(CZ // 8):
        start = 4 + 32 * group
        parts = [
            source_ref[pl.ds(source_row + start + channel, 8, stride=4), :] for channel in range(4)
        ]
        bounds = None
        if group in (0, CZ // 8 - 1):
            bounds = bounds_z(place[2] * CZ + 8 * group + sublane, width[2])
        values = velocities(parts, floor, bounds)
        for channel in range(3):
            u_ref[pl.ds(spot * PLANE + start + channel, 8, stride=4), :] = values[channel]
            if out_step is not None:
                out_ref[channel, out_step, 8 * group : 8 * group + 8, :] = roll(
                    values[channel], -1
                )[:, 0:CY]


def settle_edges(source_ref, source_row, u_ref, first, count, spot=None):
    spot = first if spot is None else spot
    place, width, low_y = place_bounds()
    sublane = lax.broadcasted_iota(jnp.int32, (8, BLOCK), 0)
    at_x = lax.rem(place[0] * CX + first + sublane - 1 + width[0], width[0])
    floor = floor_of(at_x, width[0], low_y)
    for edge in (0, CZ + 1):
        at_z = lax.rem(place[2] * CZ + edge - 1 + width[2], width[2])
        bounds = bounds_z(at_z + 0 * sublane, width[2])
        parts = [
            source_ref[pl.ds(source_row + 4 * edge + channel, count, stride=PLANE), :]
            for channel in range(4)
        ]
        values = velocities(parts, floor[0:count], [bound[0:count] for bound in bounds])
        for channel in range(3):
            start = spot * PLANE + 4 * edge + channel
            u_ref[pl.ds(start, count, stride=PLANE), :] = values[channel]


def settle_kernel(grid_ref, spread_ref, out_ref, matrix_ref, u_ref):
    def plane(step, carry):
        row = pl.multiple_of(step * PLANE, 8)
        settle_plane(grid_ref, row, u_ref, step, out_ref, step - 1)
        return carry

    matrix_ref[...] = expansion()
    lax.fori_loop(2, CX, plane, 0, unroll=7)
    for first in range(2, CX, 8):
        count = min(8, CX - first)
        settle_edges(grid_ref, first * PLANE, u_ref, first, count)

    def spread(step, carry):
        row = pl.multiple_of(step * PLANE, 8)
        expand(u_ref[pl.ds(row, PLANE), :], matrix_ref[...], spread_ref, row)
        return carry

    lax.fori_loop(2, CX, spread, 0, unroll=7)


def collect_kernel(
    blocks,
    tile_hbm,
    above_ref,
    below_ref,
    frac_ref,
    offset_ref,
    grid_ref,
    inner_ref,
    matrix_ref,
    _,
    spread_ref,
    out_hbm,
    velocity_hbm,
    affine_hbm,
    edge_ref,
    u_ref,
    out_ref,
    stage_ref,
    velocity_ref,
    affine_ref,
    tile_ref,
    sems,
):
    tile_copy = pltpu.make_async_copy(tile_hbm, tile_ref, sems.at[3 + 2 * (blocks // CHUNK)])
    tile_copy.start()
    inner = pltpu.make_async_copy(
        inner_ref.at[:, pl.ds(1, CX - 2)], out_hbm.at[:, pl.ds(1, CX - 2)], sems.at[2]
    )
    inner.start()
    for source, start, spot in ((below_ref, 0, 0), (above_ref, CX, 2)):
        first, second = unpack_pairs(source, FACE)
        for tile, value in enumerate(first + second):
            edge_ref[tile_rows(spot * FACE + tile), :] = (
                grid_ref[tile_rows(start * FACE + tile), :] + value
            )
    for spot, step in enumerate((0, 1, CX, CX + 1)):
        out_step = {1: 0, CX: 1}.get(step)
        settle_plane(edge_ref, spot * PLANE, u_ref, step, out_ref, out_step, spot)
    settle_edges(edge_ref, 0, u_ref, 0, 2)
    settle_edges(edge_ref, 2 * PLANE, u_ref, CX, 2, 2)
    matrix = matrix_ref[...]
    for spot, step in ((0, 0), (2, CX)):
        values = u_ref[spot * PLANE : (spot + 2) * PLANE, :]
        expand(values, matrix, spread_ref, step * PLANE)
    copies = [
        pltpu.make_async_copy(
            out_ref.at[:, pl.ds(slot, 1)],
            out_hbm.at[:, pl.ds(slot * (CX - 1), 1)],
            sems.at[slot],
        )
        for slot in range(2)
    ]
    for copy in copies:
        copy.start()
    copies.append(inner)

    def one_block(block):
        lanes = pl.ds(pl.multiple_of(block * BLOCK, BLOCK), BLOCK)
        corner, corner_y = tile_corner(tile_ref[block])
        fraction, offset = point_rows(frac_ref, offset_ref, lanes)
        weight_x, first_x = x_weights(fraction[0], offset[0])
        weight_z, first_z = pair_weights(fraction[2], offset[2])
        weight_y, first_y = lane_weights(fraction[1], offset[1])
        right_high, right_low = split(jnp.concatenate([weight_y, first_y], axis=1))
        right_high = right_high.astype(jnp.float32)
        fill = jnp.zeros((BLOCK - 16, 2 * BLOCK), jnp.float32)
        right_one = jnp.concatenate([right_high, right_high, fill], axis=0)
        right_two = jnp.concatenate(
            [right_low.astype(jnp.float32), jnp.zeros_like(right_high), fill], axis=0
        )
        half = corner_y // 32
        corner = corner + half * (PX * PLANE)
        turn = (128 - 4 * (corner_y - 32 * half)) & 127
        left = jnp.concatenate(
            [pltpu.roll(spread_ref[window_rows(corner, step), :], turn, 1) for step in range(6)],
            axis=0,
        ).astype(jnp.bfloat16)

        def dot(right):
            return jnp.dot(
                left, right.astype(jnp.bfloat16), preferred_element_type=jnp.float32
            )

        sums = dot(right_one) + dot(right_two)

        def over_x(weights, column):
            result = []
            for pair in range(3):
                total = None
                for step in range(6):
                    row = 24 * step + 8 * pair
                    term = weights[step] * sums[row : row + 8, column : column + BLOCK]
                    total = term if total is None else total + term
                result.append(total)
            return result

        def over_z(weights, values):
            total = weights[0] * values[0] + weights[1] * values[1] + weights[2] * values[2]
            return total + pltpu.roll(total, 4, 0)

        plain = over_x(weight_x, 0)
        velocity = over_z(weight_z, plain)
        columns = (
            over_z(weight_z, over_x(first_x, 0)),
            over_z(weight_z, over_x(weight_x, BLOCK)),
            over_z(first_z, plain),
        )
        return block, lanes, velocity, columns

    chunk_count = blocks // CHUNK
    tile_copy.wait()

    def chunk_copies(chunk):
        part = pl.ds(pl.multiple_of(chunk * (CHUNK * BLOCK), BLOCK), CHUNK * BLOCK)
        return [
            pltpu.make_async_copy(
                source.at[:, part], target.at[:, part], sems.at[3 + side * chunk_count + chunk]
            )
            for side, (source, target) in enumerate(
                ((velocity_ref, velocity_hbm), (affine_ref, affine_hbm))
            )
        ]

    def one_chunk(chunk, carry):
        results = [one_block(chunk * CHUNK + spot) for spot in range(CHUNK)]
        for block, lanes, velocity, columns in results:
            velocity_ref[:, lanes] = velocity[0:3]
            for col in range(3):
                stage_ref[pl.ds(block * 16 + col, 3, stride=3), :] = 4.0 * columns[col][0:3]
        for block, lanes, _, _ in results:
            affine_ref[:, lanes] = stage_ref[pl.ds(pl.multiple_of(block * 16, 8), 9), :]
        for copy in chunk_copies(chunk):
            copy.start()
        return carry

    lax.fori_loop(0, chunk_count, one_chunk, 0)
    for chunk in range(chunk_count):
        copies += chunk_copies(chunk)
    for copy in copies:
        copy.wait()


def exchange(low, high, axis):
    count = lax.axis_size(axis)
    up = [(i, (i + 1) % count) for i in range(count)]
    down = [(target, source) for source, target in up]
    return lax.ppermute(low, axis, down), lax.ppermute(high, axis, up)


def shards(
    point_frac,
    cell_offset,
    point_velocity,
    point_affine,
    point_stress,
    point_mass,
    block_tile,
    block_count,
):
    blocks = block_tile.shape[0]
    points = blocks * BLOCK
    f32 = jnp.float32
    vmem = pl.BlockSpec(memory_space=pltpu.VMEM)
    hbm = pl.BlockSpec(memory_space=pltpu.HBM)
    params = pltpu.CompilerParams(vmem_limit_bytes=VMEM_LIMIT)
    grid_shape = jax.ShapeDtypeStruct((ROWS, BLOCK), f32)
    out_shape = jax.ShapeDtypeStruct((3, CX, CZ, CY), f32)

    def message(tiles):
        return jax.ShapeDtypeStruct((8 * tiles, BLOCK), f32)

    def cost(microseconds):
        return pl.CostEstimate(
            flops=int(microseconds * 8.0e6), bytes_accessed=1000, transcendentals=0
        )

    mass = point_mass.reshape(blocks, BLOCK)
    inputs = (
        block_tile,
        block_count,
        point_frac,
        cell_offset,
        point_velocity,
        point_affine,
        point_stress,
        mass,
    )
    new_stress, grid, low, high = pl.pallas_call(
        lambda *refs: deposit_kernel(blocks, *refs),
        out_shape=(
            jax.ShapeDtypeStruct((6, points), f32),
            grid_shape,
            message(SPAN),
            message(SPAN),
        ),
        in_specs=[hbm] * 8,
        out_specs=(hbm, vmem, vmem, vmem),
        scratch_shapes=[
            pltpu.SMEM(block_tile.shape, jnp.int32),
            pltpu.SMEM(block_count.shape, jnp.int32),
        ]
        + [pltpu.VMEM(array.shape, array.dtype) for array in inputs[2:]]
        + [
            pltpu.VMEM((6, points), f32),
            pltpu.VMEM((50 * STRIDE, BLOCK), f32),
            pltpu.SemaphoreType.DMA((9,)),
        ],
        compiler_params=params,
        cost_estimate=cost(5),
        name="deposit",
    )(*[pltpu.with_memory_space_constraint(array, pltpu.HBM) for array in inputs])
    above, below = exchange(low, high, "gy")
    grid, low, high = pl.pallas_call(
        join_y_faces,
        out_shape=(grid_shape, message(PX // 2 + 1), message(PX // 2 + 1)),
        in_specs=[vmem] * 3,
        out_specs=(vmem,) * 3,
        input_output_aliases={2: 0},
        compiler_params=params,
        cost_estimate=cost(0.3),
        name="join_y_faces",
    )(above, below, grid)
    grid = pl.pallas_call(
        join_y_rest,
        out_shape=grid_shape,
        in_specs=[vmem] * 3,
        out_specs=vmem,
        input_output_aliases={2: 0},
        compiler_params=params,
        cost_estimate=cost(1),
        name="join_y_rest",
    )(above, below, grid)
    above, below = exchange(low, high, "gz")
    grid, low, high = pl.pallas_call(
        join_z,
        out_shape=(grid_shape, message(FACE + 1), message(FACE + 1)),
        in_specs=[vmem] * 3,
        out_specs=(vmem,) * 3,
        input_output_aliases={2: 0},
        compiler_params=params,
        cost_estimate=cost(0.3),
        name="join_z",
    )(above, below, grid)
    above, below = exchange(low, high, "gx")
    spread_shape = message(2 * TILES)
    spread, inner, matrix = pl.pallas_call(
        settle_kernel,
        out_shape=(
            spread_shape,
            out_shape,
            jax.ShapeDtypeStruct((2 * BLOCK, 2 * BLOCK), jnp.bfloat16),
        ),
        in_specs=[vmem],
        out_specs=(vmem, vmem, vmem),
        scratch_shapes=[pltpu.VMEM((PX * PLANE, BLOCK), f32)],
        compiler_params=params,
        cost_estimate=cost(2),
        name="settle",
    )(grid)
    _, grid_velocity, new_velocity, new_affine = pl.pallas_call(
        lambda *refs: collect_kernel(blocks, *refs),
        out_shape=(
            spread_shape,
            out_shape,
            jax.ShapeDtypeStruct((3, points), f32),
            jax.ShapeDtypeStruct((9, points), f32),
        ),
        in_specs=[hbm] + [vmem] * 8,
        out_specs=(vmem, hbm, hbm, hbm),
        input_output_aliases={8: 0},
        scratch_shapes=[
            pltpu.VMEM((4 * PLANE, BLOCK), f32),
            pltpu.VMEM((4 * PLANE, BLOCK), f32),
            pltpu.VMEM((3, 2, CZ, CY), f32),
            pltpu.VMEM((blocks * 16, BLOCK), f32),
            pltpu.VMEM((3, points), f32),
            pltpu.VMEM((9, points), f32),
            pltpu.SMEM(block_tile.shape, jnp.int32),
            pltpu.SemaphoreType.DMA((4 + 2 * (blocks // CHUNK),)),
        ],
        compiler_params=params,
        cost_estimate=cost(4),
        name="collect",
    )(pltpu.with_memory_space_constraint(block_tile, pltpu.HBM), above, below, point_frac, cell_offset, grid, inner, matrix, spread)
    return (new_velocity, new_affine, new_stress, grid_velocity.transpose(0, 1, 3, 2))


def solution(mesh):
    points = ("gx", "gy", "gz")
    return jax.shard_map(
        shards,
        mesh=mesh,
        in_specs=(P(None, points),) * 5 + (P(points),) * 3,
        out_specs=(P(None, points),) * 3 + (P(None, "gx", "gy", "gz"),),
        check_vma=False,
    )
```

```python
import jax
import jax.numpy as jnp
from jax import lax
from jax.experimental import pallas as pl
from jax.experimental.pallas import tpu as pltpu
from jax.sharding import PartitionSpec as P


CX = 16
CY = 64
CZ = 32
BLOCK = 128

time_step = 0.1
gravity = 1.0
shear_modulus = 2.0
bulk_modulus = 4.0
friction_static = 0.38
friction_limit = 0.64
inertial_ref = 0.28
grain_size = 0.5
grain_density = 1.0
pressure_floor = 0.5
shear_floor = 0.5
mass_floor = 0.05
stress_scale = 0.4
pair_index = ((0, 5, 4), (5, 1, 3), (4, 3, 2))
component_pairs = ((0, 0), (1, 1), (2, 2), (1, 2), (0, 2), (0, 1))

PX = CX + 2
PY = CY + 2
PZ = CZ + 2
PLANE = 4 * PZ
TILES = PX * PLANE // 8
SPAN = 5
GROUPS = -(-TILES // SPAN)
ROWS = GROUPS * SPAN * 8
REST = 2 * PY - 128
STRIDE = 40
CHUNK = 16
PARTS = 18
SEATS = BLOCK // PARTS
SPREADS = -(-(CY // 4) // SEATS)
VMEM_LIMIT = 16 * 1024 * 1024
FAR = 3.0e38


def stress_update(stress, affine):
    strain_rate = [
        [
            0.5 * (affine[3 * row_dim + col_dim] + affine[3 * col_dim + row_dim])
            for col_dim in range(3)
        ]
        for row_dim in range(3)
    ]
    volume_rate = strain_rate[0][0] + strain_rate[1][1] + strain_rate[2][2]
    deviator = [
        [
            strain_rate[row_dim][col_dim] - (volume_rate / 3.0 if row_dim == col_dim else 0.0)
            for col_dim in range(3)
        ]
        for row_dim in range(3)
    ]
    trial_stress = []
    for component in range(6):
        row_dim, col_dim = component_pairs[component]
        value = stress[component] + time_step * 2.0 * shear_modulus * deviator[row_dim][col_dim]
        if component < 3:
            value = value + time_step * bulk_modulus * volume_rate
        trial_stress.append(value)
    pressure = -(trial_stress[0] + trial_stress[1] + trial_stress[2]) / 3.0
    shear_part = [trial_stress[component] + pressure for component in range(3)] + trial_stress[3:]
    shear_stress = jnp.sqrt(
        0.5 * (shear_part[0] ** 2 + shear_part[1] ** 2 + shear_part[2] ** 2)
        + shear_part[3] ** 2
        + shear_part[4] ** 2
        + shear_part[5] ** 2
    )
    shear_rate = jnp.sqrt(
        2.0
        * (
            deviator[0][0] ** 2
            + deviator[1][1] ** 2
            + deviator[2][2] ** 2
            + 2.0 * (deviator[1][2] ** 2 + deviator[0][2] ** 2 + deviator[0][1] ** 2)
        )
    )
    inertial = (
        shear_rate * grain_size / jnp.sqrt(jnp.maximum(pressure, pressure_floor) / grain_density)
    )
    friction = friction_static + (friction_limit - friction_static) * inertial / (
        inertial_ref + inertial
    )
    support = jnp.maximum(pressure, 0.0)
    factor = jnp.minimum(1.0, friction * support / jnp.maximum(shear_stress, shear_floor))
    return [shear_part[component] * factor - support for component in range(3)] + [
        shear_part[component] * factor for component in range(3, 6)
    ]


def spline(fraction):
    left = 0.5 * (1.5 - fraction) ** 2
    middle = 0.75 - (fraction - 1.0) ** 2
    right = 0.5 * (fraction - 0.5) ** 2
    plain = (left, middle, right)
    moment = (left * (0.0 - fraction), middle * (1.0 - fraction), right * (2.0 - fraction))
    return plain, moment


def pick(masks, values):
    zero = jnp.zeros_like(values[0])
    return jnp.where(
        masks[0], values[0], jnp.where(masks[1], values[1], jnp.where(masks[2], values[2], zero))
    )


def slot_masks(slot, offset):
    shifted = slot - offset
    return (shifted == 0, shifted == 1, shifted == 2)


def x_weights(fraction, offset):
    plain, moment = spline(fraction)
    at = [offset == step for step in range(4)]
    zero = jnp.zeros_like(fraction)
    result = []
    for values in (plain, moment):
        row = []
        for slot in range(6):
            value = zero
            for node in range(3):
                if 0 <= slot - node <= 3:
                    value = jnp.where(at[slot - node], values[node], value)
            row.append(value)
        result.append(row)
    return result


def pair_weights(fraction, offset):
    plain, moment = spline(fraction)
    upper = (lax.broadcasted_iota(jnp.int32, (8, BLOCK), 0) >= 4).astype(jnp.int32)
    weight, first = [], []
    for pair in range(3):
        masks = slot_masks(upper + 2 * pair, offset)
        weight.append(pick(masks, plain))
        first.append(pick(masks, moment))
    return weight, first


def lane_weights(fraction, offset):
    plain, moment = spline(fraction)
    slot = lax.broadcasted_iota(jnp.int32, (8, BLOCK), 0)
    masks = slot_masks(slot, offset)
    return pick(masks, plain), pick(masks, moment)


def split(values):
    high = values.astype(jnp.bfloat16)
    return high, (values - high.astype(jnp.float32)).astype(jnp.bfloat16)


def point_rows(frac_ref, offset_ref, lanes):
    fraction = [jnp.broadcast_to(frac_ref[dim : dim + 1, lanes], (8, BLOCK)) for dim in range(3)]
    offset = [jnp.broadcast_to(offset_ref[dim : dim + 1, lanes], (8, BLOCK)) for dim in range(3)]
    return fraction, offset


def tile_corner(tile):
    tiles_y, tiles_z = CY // 4, CZ // 4
    tile_x = tile // (tiles_y * tiles_z)
    tile_y = (tile // tiles_z) % tiles_y
    tile_z = tile % tiles_z
    return tile_x * (4 * PLANE) + tile_z * 16, tile_y * 4


def expansion():
    row = lax.broadcasted_iota(jnp.int32, (2 * BLOCK, SPREADS * BLOCK), 0)
    col = lax.broadcasted_iota(jnp.int32, (2 * BLOCK, SPREADS * BLOCK), 1)
    tile = (col // BLOCK) * SEATS + (col % BLOCK) // PARTS
    part = (col % BLOCK) % PARTS
    source = 4 * tile + part % 6 + jnp.where(part // 6 == 1, BLOCK, 0)
    seated = (col % BLOCK < SEATS * PARTS) & (tile < CY // 4)
    return jnp.where((row == source) & seated, 1.0, 0.0).astype(jnp.bfloat16)


def expand(values, matrix, spread_ref, row):
    wide = jnp.dot(
        jnp.concatenate(split(values), axis=1), matrix, preferred_element_type=jnp.float32
    )
    count = values.shape[0]
    for spread in range(SPREADS):
        rows = pl.ds(pl.multiple_of(row + spread * PX * PLANE, 8), count)
        spread_ref[rows, :] = wide[:, spread * BLOCK : (spread + 1) * BLOCK]


def window_rows(corner, step):
    return pl.ds(pl.multiple_of(corner + step * PLANE, 8), 24)


def lane_index():
    return lax.broadcasted_iota(jnp.int32, (8, BLOCK), 1)


def roll(values, shift):
    return pltpu.roll(values, shift % 128, 1) if shift % 128 else values


def pack_pairs(first, second, target, start=0):
    lane = lane_index()
    last = jnp.zeros((8, BLOCK), jnp.float32)
    for spot, (one, two) in enumerate(zip(first, second)):
        target[tile_rows(start + spot), :] = jnp.where(lane < PY, one, roll(two, PY))
        last = jnp.where(lane // REST == spot, roll(two, REST * spot - (PY - REST)), last)
    target[tile_rows(start + len(first)), :] = last


def unpack_pairs(source, count, start=0):
    lane = lane_index()
    last = source[tile_rows(start + count), :]
    first, second = [], []
    for spot in range(count):
        tile = source[tile_rows(start + spot), :]
        first.append(jnp.where(lane < PY, tile, 0.0))
        tail = jnp.where(lane < PY, roll(last, (PY - REST) - REST * spot), 0.0)
        second.append(jnp.where(lane < PY - REST, roll(tile, -PY), tail))
    return first, second


def tile_rows(tile):
    return slice(8 * tile, 8 * tile + 8)


def deposit_kernel(
    blocks,
    tile_hbm,
    count_hbm,
    frac_hbm,
    offset_hbm,
    velocity_hbm,
    affine_hbm,
    stress_hbm,
    mass_hbm,
    stress_out,
    grid_ref,
    low_ref,
    high_ref,
    early_ref,
    tile_ref,
    count_ref,
    frac_ref,
    offset_ref,
    velocity_ref,
    affine_ref,
    stress_ref,
    mass_ref,
    new_stress_ref,
    dense_ref,
    sems,
):
    sources = (
        velocity_hbm,
        affine_hbm,
        stress_hbm,
        mass_hbm,
        tile_hbm,
        count_hbm,
        frac_hbm,
        offset_hbm,
    )
    targets = (
        velocity_ref,
        affine_ref,
        stress_ref,
        mass_ref,
        tile_ref,
        count_ref,
        frac_ref,
        offset_ref,
    )
    copies = [
        pltpu.make_async_copy(source, target, sems.at[slot])
        for slot, (source, target) in enumerate(zip(sources, targets))
    ]
    for copy in copies:
        copy.start()
    grid_ref[...] = jnp.zeros_like(grid_ref)
    for copy in copies:
        copy.wait()

    def dense(component):
        return dense_ref[component * STRIDE : component * STRIDE + blocks, :]

    def put(component, values):
        dense_ref[component * STRIDE : component * STRIDE + blocks, :] = values

    for block in range(blocks):
        lanes = slice(block * BLOCK, (block + 1) * BLOCK)
        dense_ref[pl.ds(block, 3, stride=STRIDE), :] = velocity_ref[:, lanes]
        dense_ref[pl.ds(3 * STRIDE + block, 9, stride=STRIDE), :] = affine_ref[:, lanes]
        dense_ref[pl.ds(12 * STRIDE + block, 6, stride=STRIDE), :] = stress_ref[:, lanes]
    velocity = [dense(component) for component in range(3)]
    affine = [dense(3 + component) for component in range(9)]
    stress = [dense(12 + component) for component in range(6)]
    new_stress = stress_update(stress, affine)
    for component in range(6):
        put(12 + component, new_stress[component])
    mass = mass_ref[...]
    columns = [[mass * velocity[row] for row in range(3)] + [mass]]
    for col in range(3):
        columns.append(
            [
                mass * (affine[3 * row + col] - stress_scale * new_stress[pair_index[row][col]])
                for row in range(3)
            ]
            + [jnp.zeros_like(mass)]
        )
    for group in range(4):
        for channel in range(4):
            put(18 + 8 * group + channel, columns[group][channel])
            put(18 + 8 * group + 4 + channel, columns[group][channel])
    for block in range(blocks):
        lanes = slice(block * BLOCK, (block + 1) * BLOCK)
        new_stress_ref[:, lanes] = dense_ref[pl.ds(12 * STRIDE + block, 6, stride=STRIDE), :]
    stress_copy = pltpu.make_async_copy(new_stress_ref, stress_out, sems.at[len(copies)])
    stress_copy.start()

    lane = lane_index()

    def one_block(block, carry):
        lanes = pl.ds(pl.multiple_of(block * BLOCK, BLOCK), BLOCK)
        corner, corner_y = tile_corner(tile_ref[block])
        fraction, offset = point_rows(frac_ref, offset_ref, lanes)
        base, col_x, col_y, col_z = [
            dense_ref[pl.ds((18 + 8 * group) * STRIDE + block, 8, stride=STRIDE), :]
            for group in range(4)
        ]
        weight_x, first_x = x_weights(fraction[0], offset[0])
        weight_z, first_z = pair_weights(fraction[2], offset[2])
        offset_y = jnp.where(lane < count_ref[block], offset[1], -100)
        weight_y, first_y = lane_weights(fraction[1], offset_y)
        right = jnp.concatenate([weight_y, first_y], axis=1)
        flat = [base * weight_z[pair] + col_z * first_z[pair] for pair in range(3)]
        along = [col_x * weight_z[pair] for pair in range(3)]
        depth = [col_y * weight_z[pair] for pair in range(3)]
        left = jnp.concatenate(
            [
                jnp.concatenate(
                    [
                        weight_x[step] * flat[pair] + first_x[step] * along[pair]
                        for step in range(6)
                        for pair in range(3)
                    ],
                    axis=0,
                ),
                jnp.concatenate(
                    [weight_x[step] * depth[pair] for step in range(6) for pair in range(3)],
                    axis=0,
                ),
            ],
            axis=1,
        )
        left_high, left_low = split(left)
        fill = jnp.zeros((BLOCK - 8, 2 * BLOCK), jnp.float32)
        right_high, right_low = split(jnp.concatenate([right, fill], axis=0))

        def dot(one, two):
            return lax.dot_general(
                one, two, (((1,), (1,)), ((), ())), preferred_element_type=jnp.float32
            )

        sums = dot(left_high, right_high) + dot(left_low, right_high) + dot(left_high, right_low)
        for step in range(6):
            rows = window_rows(corner, step)
            grid_ref[rows, :] += pltpu.roll(sums[24 * step : 24 * step + 24], corner_y, 1)
        return carry

    lax.fori_loop(0, blocks, one_block, 0, unroll=min(blocks, 32))

    low = [jnp.zeros((8, BLOCK), jnp.float32) for _ in range(SPAN)]
    high = [jnp.zeros((8, BLOCK), jnp.float32) for _ in range(SPAN)]
    for group in range(GROUPS):
        low_mask = lane // 2 == group
        high_mask = lane // 2 == (CY // 2 + group) % 64
        for spot in range(SPAN):
            tile = group * SPAN + spot
            if tile < TILES:
                turned = roll(grid_ref[tile_rows(tile), :], 2 * group)
                low[spot] = jnp.where(low_mask, turned, low[spot])
                high[spot] = jnp.where(high_mask, turned, high[spot])
    for spot in range(SPAN):
        low_ref[tile_rows(spot), :] = low[spot]
        high_ref[tile_rows(spot), :] = high[spot]
    for side, start in enumerate((0, CX)):
        planes = [
            [grid_ref[tile_rows((start + part) * FACE + spot), :] for spot in range(FACE)]
            for part in range(2)
        ]
        pack_pairs(planes[0], planes[1], early_ref, side * (FACE + 1))
    stress_copy.wait()


def add_y(grid_ref, above, below, tiles):
    lane = lane_index()
    bottom, top = lane // 2 == 0, lane // 2 == CY // 2
    for tile in tiles:
        group, spot = divmod(tile, SPAN)
        lower = roll(below[spot], -CY - 2 * group)
        upper = roll(above[spot], CY - 2 * group)
        grid_ref[tile_rows(tile), :] += jnp.where(bottom, lower, jnp.where(top, upper, 0.0))


FACE = PLANE // 8


RIM_TILES = [(part, spot) for part in range(2) for spot in range(1, FACE - 1)]


def join_y_faces(above_ref, below_ref, _, grid_ref, low_ref, high_ref):
    above = [above_ref[tile_rows(spot), :] for spot in range(SPAN)]
    below = [below_ref[tile_rows(spot), :] for spot in range(SPAN)]
    tiles = [step * FACE + side for step in range(PX) for side in (0, FACE - 1)]
    add_y(grid_ref, above, below, tiles)
    half = PX // 2
    for target, side in ((low_ref, 0), (high_ref, FACE - 1)):
        faces = [grid_ref[tile_rows(step * FACE + side), :] for step in range(PX)]
        pack_pairs(faces[:half], faces[half:], target)


def join_y_rest(above_ref, below_ref, _, grid_ref):
    above = [above_ref[tile_rows(spot), :] for spot in range(SPAN)]
    below = [below_ref[tile_rows(spot), :] for spot in range(SPAN)]
    tiles = [step * FACE + side for step in range(PX) for side in range(1, FACE - 1)]
    add_y(grid_ref, above, below, tiles)


def join_z(above_ref, below_ref, _, grid_ref, late_ref):
    half = PX // 2
    for source, side in ((below_ref, 0), (above_ref, FACE - 1)):
        first, second = unpack_pairs(source, half)
        for step, value in enumerate(first + second):
            grid_ref[tile_rows(step * FACE + side), :] += value
    lane = lane_index()
    for place, start in enumerate((0, CX)):

        def tile(part, spot):
            return grid_ref[tile_rows((start + part) * FACE + spot), :]

        rim = jnp.zeros((8, BLOCK), jnp.float32)
        for seat, (part, spot) in enumerate(RIM_TILES):
            rim = jnp.where(lane // 2 % 32 == seat, roll(tile(part, spot), 2 * seat), rim)
        for side, spot in enumerate((0, FACE - 1)):
            one, two = tile(0, spot), tile(1, spot)
            tail = lane // REST == 15 + 16 * side
            rim = jnp.where(tail, roll(two, 64 * side - 2), rim)
            late_ref[tile_rows(3 * place + 1 + side), :] = jnp.where(
                lane < PY, one, roll(two, PY)
            )
        late_ref[tile_rows(3 * place), :] = rim


def rim_lanes(lane):
    return (lane // 2) % (CY // 2) == 0


def late_planes(source, start):
    lane = lane_index()
    mask = rim_lanes(lane) & (lane < PY)
    rim = source[tile_rows(start), :]
    planes = [[None] * FACE for _ in range(2)]
    for seat, (part, spot) in enumerate(RIM_TILES):
        planes[part][spot] = jnp.where(mask, roll(rim, -2 * seat), 0.0)
    for side, spot in enumerate((0, FACE - 1)):
        tile = source[tile_rows(start + 1 + side), :]
        tail = jnp.where(lane < PY, roll(rim, 2 - 64 * side), 0.0)
        planes[0][spot] = jnp.where(lane < PY, tile, 0.0)
        planes[1][spot] = jnp.where(lane < PY - REST, roll(tile, -PY), tail)
    return planes


def place_bounds():
    axes = ("gx", "gy", "gz")
    place = [lax.axis_index(axis) for axis in axes]
    width = [lax.axis_size(axis) * cells for axis, cells in zip(axes, (CX, CY, CZ))]
    at_y = lax.rem(place[1] * CY + lane_index() - 1 + width[1], width[1])
    return place, width, at_y < 2


def floor_of(at_x, width_x, low_y):
    outlet = (at_x >= width_x // 4) & (at_x < width_x - width_x // 4)
    return jnp.where(low_y & jnp.logical_not(outlet), 0.0, -FAR)


def bounds_z(at_z, depth_z):
    return jnp.where(at_z < 2, 0.0, -FAR), jnp.where(at_z >= depth_z - 2, 0.0, FAR)


def velocities(parts, floor, bounds):
    inverse = 1.0 / (parts[3] + mass_floor)
    u_x = parts[0] * inverse
    u_y = jnp.maximum(parts[1] * inverse - time_step * gravity, floor)
    u_z = parts[2] * inverse
    if bounds is not None:
        u_z = jnp.minimum(jnp.maximum(u_z, bounds[0]), bounds[1])
    return u_x, u_y, u_z


def settle_plane(source_ref, source_row, u_ref, step, out_ref, out_step, spot=None):
    spot = step if spot is None else spot
    place, width, low_y = place_bounds()
    sublane = lax.broadcasted_iota(jnp.int32, (8, BLOCK), 0)
    at_x = lax.rem(place[0] * CX + step - 1 + width[0], width[0])
    floor = floor_of(at_x, width[0], low_y)
    for group in range(CZ // 8):
        start = 4 + 32 * group
        parts = [
            source_ref[pl.ds(source_row + start + channel, 8, stride=4), :] for channel in range(4)
        ]
        bounds = None
        if group in (0, CZ // 8 - 1):
            bounds = bounds_z(place[2] * CZ + 8 * group + sublane, width[2])
        values = velocities(parts, floor, bounds)
        for channel in range(3):
            u_ref[pl.ds(spot * PLANE + start + channel, 8, stride=4), :] = values[channel]
            if out_step is not None:
                out_ref[channel, out_step, 8 * group : 8 * group + 8, :] = roll(
                    values[channel], -1
                )[:, 0:CY]


def settle_edges(source_ref, source_row, u_ref, first, count, spot=None):
    spot = first if spot is None else spot
    place, width, low_y = place_bounds()
    sublane = lax.broadcasted_iota(jnp.int32, (8, BLOCK), 0)
    at_x = lax.rem(place[0] * CX + first + sublane - 1 + width[0], width[0])
    floor = floor_of(at_x, width[0], low_y)
    for edge in (0, CZ + 1):
        at_z = lax.rem(place[2] * CZ + edge - 1 + width[2], width[2])
        bounds = bounds_z(at_z + 0 * sublane, width[2])
        parts = [
            source_ref[pl.ds(source_row + 4 * edge + channel, count, stride=PLANE), :]
            for channel in range(4)
        ]
        values = velocities(parts, floor[0:count], [bound[0:count] for bound in bounds])
        for channel in range(3):
            start = spot * PLANE + 4 * edge + channel
            u_ref[pl.ds(start, count, stride=PLANE), :] = values[channel]


def settle_kernel(
    source_ref, grid_ref, spread_ref, out_ref, matrix_ref, edge_ref, u_ref
):
    rim = rim_lanes(lane_index())
    for side, start, place in ((1, 0, 0), (0, CX, 2)):
        for part, tiles in enumerate(unpack_pairs(source_ref, FACE, side * (FACE + 1))):
            for spot, value in enumerate(tiles):
                mine = grid_ref[tile_rows((start + part) * FACE + spot), :]
                if 0 < spot < FACE - 1:
                    mine = mine + jnp.where(rim, 0.0, value)
                edge_ref[tile_rows((place + part) * FACE + spot), :] = mine

    def plane(step, carry):
        row = pl.multiple_of(step * PLANE, 8)
        settle_plane(grid_ref, row, u_ref, step, out_ref, step - 1)
        return carry

    matrix_ref[...] = expansion()
    lax.fori_loop(2, CX, plane, 0, unroll=7)
    for first in range(2, CX, 8):
        count = min(8, CX - first)
        settle_edges(grid_ref, first * PLANE, u_ref, first, count)

    def spread(step, carry):
        row = pl.multiple_of(step * PLANE, 8)
        expand(u_ref[pl.ds(row, PLANE), :], matrix_ref[...], spread_ref, row)
        return carry

    lax.fori_loop(2, CX, spread, 0, unroll=7)


def weights_kernel(blocks, frac_ref, offset_ref, x_ref, z_ref, y_ref):
    for block in range(blocks):
        lanes = slice(block * BLOCK, (block + 1) * BLOCK)
        fraction, offset = point_rows(frac_ref, offset_ref, lanes)
        for side, values in enumerate(lane_weights(fraction[0], offset[0])):
            x_ref[tile_rows(2 * block + side), :] = values
        weight_z, first_z = pair_weights(fraction[2], offset[2])
        for spot, values in enumerate(weight_z + first_z):
            z_ref[tile_rows(6 * block + spot), :] = values
        plain, moment = spline(fraction[1])
        slot = lax.broadcasted_iota(jnp.int32, (8, BLOCK), 0)
        pieces = []
        for group in range(3):
            row = slot + 8 * group
            masks = slot_masks(jnp.where(row < PARTS, row % 6, -100), offset[1])
            values = jnp.concatenate([pick(masks, plain), pick(masks, moment)], axis=1)
            high, low = split(values)
            wide = lax.broadcasted_iota(jnp.int32, values.shape, 0) + 8 * group
            pieces.append(
                jnp.where(wide < 12, high.astype(jnp.float32), low.astype(jnp.float32))
            )
        pieces.append(jnp.zeros_like(pieces[0]))
        y_ref[32 * block : 32 * block + 32, :] = jnp.concatenate(pieces, axis=0).astype(
            jnp.bfloat16
        )


def collect_kernel(
    blocks,
    tile_vmem,
    late_ref,
    x_ref,
    z_ref,
    y_ref,
    early_ref,
    inner_ref,
    matrix_ref,
    _,
    spread_ref,
    out_hbm,
    velocity_hbm,
    affine_hbm,
    edge_ref,
    u_ref,
    out_ref,
    stage_ref,
    velocity_ref,
    affine_ref,
    tile_ref,
    sems,
):
    tile_copy = pltpu.make_async_copy(tile_vmem, tile_ref, sems.at[3 + 2 * (blocks // CHUNK)])
    tile_copy.start()
    inner = pltpu.make_async_copy(
        inner_ref.at[:, pl.ds(1, CX - 2)], out_hbm.at[:, pl.ds(1, CX - 2)], sems.at[2]
    )
    inner.start()
    for side, place in ((1, 0), (0, 2)):
        for part, tiles in enumerate(late_planes(late_ref, 3 * side)):
            for spot, value in enumerate(tiles):
                rows = tile_rows((place + part) * FACE + spot)
                edge_ref[rows, :] = early_ref[rows, :] + value
    for spot, step in enumerate((0, 1, CX, CX + 1)):
        out_step = {1: 0, CX: 1}.get(step)
        settle_plane(edge_ref, spot * PLANE, u_ref, step, out_ref, out_step, spot)
    settle_edges(edge_ref, 0, u_ref, 0, 2)
    settle_edges(edge_ref, 2 * PLANE, u_ref, CX, 2, 2)
    matrix = matrix_ref[...]
    for spot, step in ((0, 0), (2, CX)):
        values = u_ref[spot * PLANE : (spot + 2) * PLANE, :]
        expand(values, matrix, spread_ref, step * PLANE)
    copies = [
        pltpu.make_async_copy(
            out_ref.at[:, pl.ds(slot, 1)],
            out_hbm.at[:, pl.ds(slot * (CX - 1), 1)],
            sems.at[slot],
        )
        for slot in range(2)
    ]
    for copy in copies:
        copy.start()
    copies.append(inner)

    def one_block(block):
        lanes = pl.ds(pl.multiple_of(block * BLOCK, BLOCK), BLOCK)
        corner, corner_y = tile_corner(tile_ref[block])

        def x_row(slot):
            return x_ref[pl.ds(block * 16 + slot, 8, stride=0), :]

        def z_tile(slot):
            return z_ref[pl.ds(pl.multiple_of(block * 48 + 8 * slot, 8), 8), :]

        weight_x = [x_row(slot) for slot in range(6)]
        first_x = [x_row(8 + slot) for slot in range(6)]
        weight_z = [z_tile(slot) for slot in range(3)]
        first_z = [z_tile(3 + slot) for slot in range(3)]
        right = y_ref[pl.ds(pl.multiple_of(block * 32, 32), 32), :]
        seat = corner_y // 4
        spread = seat // SEATS
        corner = corner + spread * (PX * PLANE)
        turn = (128 - PARTS * (seat - spread * SEATS)) & 127
        left = jnp.concatenate(
            [pltpu.roll(spread_ref[window_rows(corner, step), :], turn, 1) for step in range(6)],
            axis=0,
        ).astype(jnp.bfloat16)

        sums = jnp.dot(left[:, 0:24], right[0:24], preferred_element_type=jnp.float32)

        def over_x(weights, column):
            result = []
            for pair in range(3):
                total = None
                for step in range(6):
                    row = 24 * step + 8 * pair
                    term = weights[step] * sums[row : row + 8, column : column + BLOCK]
                    total = term if total is None else total + term
                result.append(total)
            return result

        def over_z(weights, values):
            total = weights[0] * values[0] + weights[1] * values[1] + weights[2] * values[2]
            return total + pltpu.roll(total, 4, 0)

        plain = over_x(weight_x, 0)
        velocity = over_z(weight_z, plain)
        columns = (
            over_z(weight_z, over_x(first_x, 0)),
            over_z(weight_z, over_x(weight_x, BLOCK)),
            over_z(first_z, plain),
        )
        return block, lanes, velocity, columns

    chunk_count = blocks // CHUNK
    tile_copy.wait()

    def chunk_copies(chunk):
        part = pl.ds(pl.multiple_of(chunk * (CHUNK * BLOCK), BLOCK), CHUNK * BLOCK)
        return [
            pltpu.make_async_copy(
                source.at[:, part], target.at[:, part], sems.at[3 + side * chunk_count + chunk]
            )
            for side, (source, target) in enumerate(
                ((velocity_ref, velocity_hbm), (affine_ref, affine_hbm))
            )
        ]

    def one_chunk(chunk, carry):
        results = [one_block(chunk * CHUNK + spot) for spot in range(CHUNK)]
        for block, lanes, velocity, columns in results:
            velocity_ref[:, lanes] = velocity[0:3]
            for col in range(3):
                stage_ref[pl.ds(block * 16 + col, 3, stride=3), :] = 4.0 * columns[col][0:3]
        for block, lanes, _, _ in results:
            affine_ref[:, lanes] = stage_ref[pl.ds(pl.multiple_of(block * 16, 8), 9), :]
        for copy in chunk_copies(chunk):
            copy.start()
        return carry

    lax.fori_loop(0, chunk_count, one_chunk, 0)
    for chunk in range(chunk_count):
        copies += chunk_copies(chunk)
    for copy in copies:
        copy.wait()


def exchange(low, high, axis):
    count = lax.axis_size(axis)
    up = [(i, (i + 1) % count) for i in range(count)]
    down = [(target, source) for source, target in up]
    above = lax.ppermute(low, axis, down)
    below = lax.ppermute(high, axis, up)
    return above, below


def exchange_both(message, axis):
    if lax.axis_size(axis) == 2:
        return lax.ppermute(message, axis, [(0, 1), (1, 0)])
    half = message.shape[0] // 2
    return jnp.concatenate(exchange(message[:half], message[half:], axis))


def step(
    point_frac,
    cell_offset,
    point_velocity,
    point_affine,
    point_stress,
    point_mass,
    block_tile,
    block_count,
):
    blocks = block_tile.shape[0]
    points = blocks * BLOCK
    f32 = jnp.float32
    vmem = pl.BlockSpec(memory_space=pltpu.VMEM)
    hbm = pl.BlockSpec(memory_space=pltpu.HBM)
    params = pltpu.CompilerParams(vmem_limit_bytes=VMEM_LIMIT)
    grid_shape = jax.ShapeDtypeStruct((ROWS, BLOCK), f32)
    out_shape = jax.ShapeDtypeStruct((3, CX, CZ, CY), f32)

    def message(tiles):
        return jax.ShapeDtypeStruct((8 * tiles, BLOCK), f32)

    def cost(microseconds):
        return pl.CostEstimate(
            flops=int(microseconds * 8.0e6), bytes_accessed=1000, transcendentals=0
        )

    mass = point_mass.reshape(blocks, BLOCK)
    inputs = (
        block_tile,
        block_count,
        point_frac,
        cell_offset,
        point_velocity,
        point_affine,
        point_stress,
        mass,
    )
    new_stress, grid, low, high, early = pl.pallas_call(
        lambda *refs: deposit_kernel(blocks, *refs),
        out_shape=(
            jax.ShapeDtypeStruct((6, points), f32),
            grid_shape,
            message(SPAN),
            message(SPAN),
            message(2 * (FACE + 1)),
        ),
        in_specs=[hbm] * 8,
        out_specs=(hbm,) + (vmem,) * 4,
        scratch_shapes=[
            pltpu.SMEM(block_tile.shape, jnp.int32),
            pltpu.SMEM(block_count.shape, jnp.int32),
        ]
        + [pltpu.VMEM(array.shape, array.dtype) for array in inputs[2:]]
        + [
            pltpu.VMEM((6, points), f32),
            pltpu.VMEM((50 * STRIDE, BLOCK), f32),
            pltpu.SemaphoreType.DMA((9,)),
        ],
        compiler_params=params,
        cost_estimate=cost(5),
        name="deposit",
    )(*[pltpu.with_memory_space_constraint(array, pltpu.HBM) for array in inputs])
    weigh = pl.pallas_call(
        lambda *refs: weights_kernel(blocks, *refs),
        out_shape=(
            message(2 * blocks),
            message(6 * blocks),
            jax.ShapeDtypeStruct((32 * blocks, 2 * BLOCK), jnp.bfloat16),
        ),
        in_specs=[vmem] * 2,
        out_specs=(vmem,) * 3,
        compiler_params=params,
        cost_estimate=cost(1),
        name="weights",
    )
    weights = weigh(point_frac, cell_offset)
    above, below = exchange(low, high, "gy")
    early = exchange_both(early, "gx")
    grid, low, high = pl.pallas_call(
        join_y_faces,
        out_shape=(grid_shape, message(PX // 2 + 1), message(PX // 2 + 1)),
        in_specs=[vmem] * 3,
        out_specs=(vmem,) * 3,
        input_output_aliases={2: 0},
        compiler_params=params,
        cost_estimate=cost(0.3),
        name="join_y_faces",
    )(above, below, grid)
    grid = pl.pallas_call(
        join_y_rest,
        out_shape=grid_shape,
        in_specs=[vmem] * 3,
        out_specs=vmem,
        input_output_aliases={2: 0},
        compiler_params=params,
        cost_estimate=cost(1),
        name="join_y_rest",
    )(above, below, grid)
    above, below = exchange(low, high, "gz")
    grid, late = pl.pallas_call(
        join_z,
        out_shape=(grid_shape, message(6)),
        in_specs=[vmem] * 3,
        out_specs=(vmem,) * 2,
        input_output_aliases={2: 0},
        compiler_params=params,
        cost_estimate=cost(0.3),
        name="join_z",
    )(above, below, grid)
    late = exchange_both(late, "gx")
    spread_shape = message(SPREADS * TILES)
    spread, inner, matrix, edge = pl.pallas_call(
        settle_kernel,
        out_shape=(
            spread_shape,
            out_shape,
            jax.ShapeDtypeStruct((2 * BLOCK, SPREADS * BLOCK), jnp.bfloat16),
            message(4 * FACE),
        ),
        in_specs=[vmem] * 2,
        out_specs=(vmem,) * 4,
        scratch_shapes=[pltpu.VMEM((PX * PLANE, BLOCK), f32)],
        compiler_params=params,
        cost_estimate=cost(2),
        name="settle",
    )(early, grid)
    _, grid_velocity, new_velocity, new_affine = pl.pallas_call(
        lambda *refs: collect_kernel(blocks, *refs),
        out_shape=(
            spread_shape,
            out_shape,
            jax.ShapeDtypeStruct((3, points), f32),
            jax.ShapeDtypeStruct((9, points), f32),
        ),
        in_specs=[vmem] * 9,
        out_specs=(vmem, hbm, hbm, hbm),
        input_output_aliases={8: 0},
        scratch_shapes=[
            pltpu.VMEM((4 * PLANE, BLOCK), f32),
            pltpu.VMEM((4 * PLANE, BLOCK), f32),
            pltpu.VMEM((3, 2, CZ, CY), f32),
            pltpu.VMEM((blocks * 16, BLOCK), f32),
            pltpu.VMEM((3, points), f32),
            pltpu.VMEM((9, points), f32),
            pltpu.SMEM(block_tile.shape, jnp.int32),
            pltpu.SemaphoreType.DMA((4 + 2 * (blocks // CHUNK),)),
        ],
        compiler_params=params,
        cost_estimate=cost(4),
        name="collect",
    )(block_tile, late, *weights, edge, inner, matrix, spread)
    return (new_velocity, new_affine, new_stress, grid_velocity.transpose(0, 1, 3, 2))


def solution(mesh):
    points = ("gx", "gy", "gz")
    return jax.shard_map(
        step,
        mesh=mesh,
        in_specs=(P(None, points),) * 5 + (P(points),) * 3,
        out_specs=(P(None, points),) * 3 + (P(None, "gx", "gy", "gz"),),
        check_vma=False,
    )
```

```python
import jax
import jax.numpy as jnp
from jax import lax
from jax.experimental import pallas as pl
from jax.experimental.pallas import tpu as pltpu
from jax.sharding import PartitionSpec as P


CX = 16
CY = 64
CZ = 32
BLOCK = 128

time_step = 0.1
gravity = 1.0
shear_modulus = 2.0
bulk_modulus = 4.0
friction_static = 0.38
friction_limit = 0.64
inertial_ref = 0.28
grain_size = 0.5
grain_density = 1.0
pressure_floor = 0.5
shear_floor = 0.5
mass_floor = 0.05
stress_scale = 0.4
pair_index = ((0, 5, 4), (5, 1, 3), (4, 3, 2))
component_pairs = ((0, 0), (1, 1), (2, 2), (1, 2), (0, 2), (0, 1))

PX = CX + 2
PY = CY + 2
PZ = CZ + 2
PLANE = 4 * PZ
TILES = PX * PLANE // 8
SPAN = 5
GROUPS = -(-TILES // SPAN)
ROWS = GROUPS * SPAN * 8
REST = 2 * PY - 128
STRIDE = 40
CHUNK = 16
PARTS = 18
SEATS = BLOCK // PARTS
SPREADS = -(-(CY // 4) // SEATS)
VMEM_LIMIT = 16 * 1024 * 1024
FAR = 3.0e38


def stress_update(stress, affine):
    strain_rate = [
        [
            0.5 * (affine[3 * row_dim + col_dim] + affine[3 * col_dim + row_dim])
            for col_dim in range(3)
        ]
        for row_dim in range(3)
    ]
    volume_rate = strain_rate[0][0] + strain_rate[1][1] + strain_rate[2][2]
    deviator = [
        [
            strain_rate[row_dim][col_dim] - (volume_rate / 3.0 if row_dim == col_dim else 0.0)
            for col_dim in range(3)
        ]
        for row_dim in range(3)
    ]
    trial_stress = []
    for component in range(6):
        row_dim, col_dim = component_pairs[component]
        value = stress[component] + time_step * 2.0 * shear_modulus * deviator[row_dim][col_dim]
        if component < 3:
            value = value + time_step * bulk_modulus * volume_rate
        trial_stress.append(value)
    pressure = -(trial_stress[0] + trial_stress[1] + trial_stress[2]) / 3.0
    shear_part = [trial_stress[component] + pressure for component in range(3)] + trial_stress[3:]
    shear_stress = jnp.sqrt(
        0.5 * (shear_part[0] ** 2 + shear_part[1] ** 2 + shear_part[2] ** 2)
        + shear_part[3] ** 2
        + shear_part[4] ** 2
        + shear_part[5] ** 2
    )
    shear_rate = jnp.sqrt(
        2.0
        * (
            deviator[0][0] ** 2
            + deviator[1][1] ** 2
            + deviator[2][2] ** 2
            + 2.0 * (deviator[1][2] ** 2 + deviator[0][2] ** 2 + deviator[0][1] ** 2)
        )
    )
    inertial = (
        shear_rate * grain_size / jnp.sqrt(jnp.maximum(pressure, pressure_floor) / grain_density)
    )
    friction = friction_static + (friction_limit - friction_static) * inertial / (
        inertial_ref + inertial
    )
    support = jnp.maximum(pressure, 0.0)
    factor = jnp.minimum(1.0, friction * support / jnp.maximum(shear_stress, shear_floor))
    return [shear_part[component] * factor - support for component in range(3)] + [
        shear_part[component] * factor for component in range(3, 6)
    ]


def spline(fraction):
    left = 0.5 * (1.5 - fraction) ** 2
    middle = 0.75 - (fraction - 1.0) ** 2
    right = 0.5 * (fraction - 0.5) ** 2
    plain = (left, middle, right)
    moment = (left * (0.0 - fraction), middle * (1.0 - fraction), right * (2.0 - fraction))
    return plain, moment


def pick(masks, values):
    zero = jnp.zeros_like(values[0])
    return jnp.where(
        masks[0], values[0], jnp.where(masks[1], values[1], jnp.where(masks[2], values[2], zero))
    )


def slot_masks(slot, offset):
    shifted = slot - offset
    return (shifted == 0, shifted == 1, shifted == 2)


def x_weights(fraction, offset):
    plain, moment = spline(fraction)
    at = [offset == step for step in range(4)]
    zero = jnp.zeros_like(fraction)
    result = []
    for values in (plain, moment):
        row = []
        for slot in range(6):
            value = zero
            for node in range(3):
                if 0 <= slot - node <= 3:
                    value = jnp.where(at[slot - node], values[node], value)
            row.append(value)
        result.append(row)
    return result


def pair_weights(fraction, offset):
    plain, moment = spline(fraction)
    upper = (lax.broadcasted_iota(jnp.int32, (8, BLOCK), 0) >= 4).astype(jnp.int32)
    weight, first = [], []
    for pair in range(3):
        masks = slot_masks(upper + 2 * pair, offset)
        weight.append(pick(masks, plain))
        first.append(pick(masks, moment))
    return weight, first


def lane_weights(fraction, offset):
    plain, moment = spline(fraction)
    slot = lax.broadcasted_iota(jnp.int32, (8, BLOCK), 0)
    masks = slot_masks(slot, offset)
    return pick(masks, plain), pick(masks, moment)


def split(values):
    high = values.astype(jnp.bfloat16)
    return high, (values - high.astype(jnp.float32)).astype(jnp.bfloat16)


def point_rows(frac_ref, offset_ref, lanes):
    fraction = [jnp.broadcast_to(frac_ref[dim : dim + 1, lanes], (8, BLOCK)) for dim in range(3)]
    offset = [jnp.broadcast_to(offset_ref[dim : dim + 1, lanes], (8, BLOCK)) for dim in range(3)]
    return fraction, offset


def tile_corner(tile):
    tiles_y, tiles_z = CY // 4, CZ // 4
    tile_x = tile // (tiles_y * tiles_z)
    tile_y = (tile // tiles_z) % tiles_y
    tile_z = tile % tiles_z
    return tile_x * (4 * PLANE) + tile_z * 16, tile_y * 4


def expansion():
    row = lax.broadcasted_iota(jnp.int32, (2 * BLOCK, SPREADS * BLOCK), 0)
    col = lax.broadcasted_iota(jnp.int32, (2 * BLOCK, SPREADS * BLOCK), 1)
    tile = (col // BLOCK) * SEATS + (col % BLOCK) // PARTS
    part = (col % BLOCK) % PARTS
    source = 4 * tile + part % 6 + jnp.where(part // 6 == 1, BLOCK, 0)
    seated = (col % BLOCK < SEATS * PARTS) & (tile < CY // 4)
    return jnp.where((row == source) & seated, 1.0, 0.0).astype(jnp.bfloat16)


def expand(values, matrix, spread_ref, row):
    wide = jnp.dot(
        jnp.concatenate(split(values), axis=1), matrix, preferred_element_type=jnp.float32
    )
    count = values.shape[0]
    for spread in range(SPREADS):
        rows = pl.ds(pl.multiple_of(row + spread * PX * PLANE, 8), count)
        spread_ref[rows, :] = wide[:, spread * BLOCK : (spread + 1) * BLOCK]


def window_rows(corner, step):
    return pl.ds(pl.multiple_of(corner + step * PLANE, 8), 24)


def lane_index():
    return lax.broadcasted_iota(jnp.int32, (8, BLOCK), 1)


def roll(values, shift):
    return pltpu.roll(values, shift % 128, 1) if shift % 128 else values


def pack_pairs(first, second, target, start=0):
    lane = lane_index()
    last = jnp.zeros((8, BLOCK), jnp.float32)
    for spot, (one, two) in enumerate(zip(first, second)):
        target[tile_rows(start + spot), :] = jnp.where(lane < PY, one, roll(two, PY))
        last = jnp.where(lane // REST == spot, roll(two, REST * spot - (PY - REST)), last)
    target[tile_rows(start + len(first)), :] = last


def unpack_pairs(source, count, start=0):
    lane = lane_index()
    last = source[tile_rows(start + count), :]
    first, second = [], []
    for spot in range(count):
        tile = source[tile_rows(start + spot), :]
        first.append(jnp.where(lane < PY, tile, 0.0))
        tail = jnp.where(lane < PY, roll(last, (PY - REST) - REST * spot), 0.0)
        second.append(jnp.where(lane < PY - REST, roll(tile, -PY), tail))
    return first, second


def tile_rows(tile):
    return slice(8 * tile, 8 * tile + 8)


def deposit_kernel(
    blocks,
    tile_hbm,
    count_hbm,
    frac_hbm,
    offset_hbm,
    velocity_hbm,
    affine_hbm,
    stress_hbm,
    mass_hbm,
    stress_out,
    grid_ref,
    low_ref,
    high_ref,
    tile_ref,
    count_ref,
    frac_ref,
    offset_ref,
    velocity_ref,
    affine_ref,
    stress_ref,
    mass_ref,
    new_stress_ref,
    dense_ref,
    sems,
):
    sources = (
        velocity_hbm,
        affine_hbm,
        stress_hbm,
        mass_hbm,
        tile_hbm,
        count_hbm,
        frac_hbm,
        offset_hbm,
    )
    targets = (
        velocity_ref,
        affine_ref,
        stress_ref,
        mass_ref,
        tile_ref,
        count_ref,
        frac_ref,
        offset_ref,
    )
    copies = [
        pltpu.make_async_copy(source, target, sems.at[slot])
        for slot, (source, target) in enumerate(zip(sources, targets))
    ]
    for copy in copies:
        copy.start()
    grid_ref[...] = jnp.zeros_like(grid_ref)
    for copy in copies:
        copy.wait()

    def dense(component):
        return dense_ref[component * STRIDE : component * STRIDE + blocks, :]

    def put(component, values):
        dense_ref[component * STRIDE : component * STRIDE + blocks, :] = values

    for block in range(blocks):
        lanes = slice(block * BLOCK, (block + 1) * BLOCK)
        dense_ref[pl.ds(block, 3, stride=STRIDE), :] = velocity_ref[:, lanes]
        dense_ref[pl.ds(3 * STRIDE + block, 9, stride=STRIDE), :] = affine_ref[:, lanes]
        dense_ref[pl.ds(12 * STRIDE + block, 6, stride=STRIDE), :] = stress_ref[:, lanes]
    velocity = [dense(component) for component in range(3)]
    affine = [dense(3 + component) for component in range(9)]
    stress = [dense(12 + component) for component in range(6)]
    new_stress = stress_update(stress, affine)
    for component in range(6):
        put(12 + component, new_stress[component])
    mass = mass_ref[...]
    columns = [[mass * velocity[row] for row in range(3)] + [mass]]
    for col in range(3):
        columns.append(
            [
                mass * (affine[3 * row + col] - stress_scale * new_stress[pair_index[row][col]])
                for row in range(3)
            ]
            + [jnp.zeros_like(mass)]
        )
    for group in range(4):
        for channel in range(4):
            put(18 + 8 * group + channel, columns[group][channel])
            put(18 + 8 * group + 4 + channel, columns[group][channel])
    for block in range(blocks):
        lanes = slice(block * BLOCK, (block + 1) * BLOCK)
        new_stress_ref[:, lanes] = dense_ref[pl.ds(12 * STRIDE + block, 6, stride=STRIDE), :]
    stress_copy = pltpu.make_async_copy(new_stress_ref, stress_out, sems.at[len(copies)])
    stress_copy.start()

    lane = lane_index()

    def one_block(block, carry):
        lanes = pl.ds(pl.multiple_of(block * BLOCK, BLOCK), BLOCK)
        corner, corner_y = tile_corner(tile_ref[block])
        fraction, offset = point_rows(frac_ref, offset_ref, lanes)
        base, col_x, col_y, col_z = [
            dense_ref[pl.ds((18 + 8 * group) * STRIDE + block, 8, stride=STRIDE), :]
            for group in range(4)
        ]
        weight_x, first_x = x_weights(fraction[0], offset[0])
        weight_z, first_z = pair_weights(fraction[2], offset[2])
        offset_y = jnp.where(lane < count_ref[block], offset[1], -100)
        weight_y, first_y = lane_weights(fraction[1], offset_y)
        right = jnp.concatenate([weight_y, first_y], axis=1)
        flat = [base * weight_z[pair] + col_z * first_z[pair] for pair in range(3)]
        along = [col_x * weight_z[pair] for pair in range(3)]
        depth = [col_y * weight_z[pair] for pair in range(3)]
        left = jnp.concatenate(
            [
                jnp.concatenate(
                    [
                        weight_x[step] * flat[pair] + first_x[step] * along[pair]
                        for step in range(6)
                        for pair in range(3)
                    ],
                    axis=0,
                ),
                jnp.concatenate(
                    [weight_x[step] * depth[pair] for step in range(6) for pair in range(3)],
                    axis=0,
                ),
            ],
            axis=1,
        )
        left_high, left_low = split(left)
        fill = jnp.zeros((BLOCK - 8, 2 * BLOCK), jnp.float32)
        right_high, right_low = split(jnp.concatenate([right, fill], axis=0))

        def dot(one, two):
            return lax.dot_general(
                one, two, (((1,), (1,)), ((), ())), preferred_element_type=jnp.float32
            )

        sums = dot(left_high, right_high) + dot(left_low, right_high) + dot(left_high, right_low)
        for step in range(6):
            rows = window_rows(corner, step)
            grid_ref[rows, :] += pltpu.roll(sums[24 * step : 24 * step + 24], corner_y, 1)
        return carry

    lax.fori_loop(0, blocks, one_block, 0, unroll=min(blocks, 32))

    half = PX // 2
    for target, side in ((low_ref, 0), (high_ref, FACE - 1)):
        faces = [grid_ref[tile_rows(step * FACE + side), :] for step in range(PX)]
        pack_pairs(faces[:half], faces[half:], target)
    stress_copy.wait()


def add_y(grid_ref, above, below, tiles):
    lane = lane_index()
    bottom, top = lane // 2 == 0, lane // 2 == CY // 2
    for tile in tiles:
        group, spot = divmod(tile, SPAN)
        lower = roll(below[spot], -CY - 2 * group)
        upper = roll(above[spot], CY - 2 * group)
        grid_ref[tile_rows(tile), :] += jnp.where(bottom, lower, jnp.where(top, upper, 0.0))


FACE = PLANE // 8


RIM_TILES = [(part, spot) for part in range(2) for spot in range(1, FACE - 1)]


def pack_y(grid_ref, low, high, tiles):
    lane = lane_index()
    for group in range(GROUPS):
        low_mask = lane // 2 == group
        high_mask = lane // 2 == (CY // 2 + group) % 64
        for spot in range(SPAN):
            tile = group * SPAN + spot
            if tile in tiles:
                turned = roll(grid_ref[tile_rows(tile), :], 2 * group)
                low[spot] = jnp.where(low_mask, turned, low[spot])
                high[spot] = jnp.where(high_mask, turned, high[spot])


Z_FACES = {step * FACE + side for step in range(PX) for side in (0, FACE - 1)}
X_EDGES = {step * FACE + spot for step in (0, 1, CX, CX + 1) for spot in range(FACE)}


def pack_kernel(grid_ref, low_ref, high_ref, early_ref):
    for side, start in enumerate((0, CX)):
        planes = [
            [grid_ref[tile_rows((start + part) * FACE + spot), :] for spot in range(FACE)]
            for part in range(2)
        ]
        pack_pairs(planes[0], planes[1], early_ref, side * (FACE + 1))
    low = [jnp.zeros((8, BLOCK), jnp.float32) for _ in range(SPAN)]
    high = [jnp.zeros((8, BLOCK), jnp.float32) for _ in range(SPAN)]
    pack_y(grid_ref, low, high, set(range(TILES)) - Z_FACES)
    for spot in range(SPAN):
        low_ref[tile_rows(spot), :] = low[spot]
        high_ref[tile_rows(spot), :] = high[spot]


def join_z(above_ref, below_ref, part_low_ref, part_high_ref, _, grid_ref, low_ref, high_ref):
    half = PX // 2
    for source, side in ((below_ref, 0), (above_ref, FACE - 1)):
        first, second = unpack_pairs(source, half)
        for step, value in enumerate(first + second):
            grid_ref[tile_rows(step * FACE + side), :] += value
    low = [part_low_ref[tile_rows(spot), :] for spot in range(SPAN)]
    high = [part_high_ref[tile_rows(spot), :] for spot in range(SPAN)]
    pack_y(grid_ref, low, high, Z_FACES)
    for spot in range(SPAN):
        low_ref[tile_rows(spot), :] = low[spot]
        high_ref[tile_rows(spot), :] = high[spot]


def read_tiles(source):
    return [source[tile_rows(spot), :] for spot in range(SPAN)]


def join_y_rest(above_ref, below_ref, _, grid_ref):
    tiles = sorted(set(range(TILES)) - X_EDGES)
    add_y(grid_ref, read_tiles(above_ref), read_tiles(below_ref), tiles)


RIM_TILES = [(part, spot) for part in range(2) for spot in range(1, FACE - 1)]


def join_y_edges(above_ref, below_ref, _, grid_ref, late_ref):
    add_y(grid_ref, read_tiles(above_ref), read_tiles(below_ref), sorted(X_EDGES))
    lane = lane_index()
    for place, start in enumerate((0, CX)):

        def tile(part, spot):
            return grid_ref[tile_rows((start + part) * FACE + spot), :]

        rim = jnp.zeros((8, BLOCK), jnp.float32)
        for seat, (part, spot) in enumerate(RIM_TILES):
            rim = jnp.where(lane // 2 % 32 == seat, roll(tile(part, spot), 2 * seat), rim)
        for side, spot in enumerate((0, FACE - 1)):
            one, two = tile(0, spot), tile(1, spot)
            tail = lane // REST == 15 + 16 * side
            rim = jnp.where(tail, roll(two, 64 * side - 2), rim)
            late_ref[tile_rows(3 * place + 1 + side), :] = jnp.where(
                lane < PY, one, roll(two, PY)
            )
        late_ref[tile_rows(3 * place), :] = rim


def rim_lanes(lane):
    return (lane // 2) % (CY // 2) == 0


def late_planes(source, start):
    lane = lane_index()
    mask = rim_lanes(lane) & (lane < PY)
    rim = source[tile_rows(start), :]
    planes = [[None] * FACE for _ in range(2)]
    for seat, (part, spot) in enumerate(RIM_TILES):
        planes[part][spot] = jnp.where(mask, roll(rim, -2 * seat), 0.0)
    for side, spot in enumerate((0, FACE - 1)):
        tile = source[tile_rows(start + 1 + side), :]
        tail = jnp.where(lane < PY, roll(rim, 2 - 64 * side), 0.0)
        planes[0][spot] = jnp.where(lane < PY, tile, 0.0)
        planes[1][spot] = jnp.where(lane < PY - REST, roll(tile, -PY), tail)
    return planes


def place_bounds():
    axes = ("gx", "gy", "gz")
    place = [lax.axis_index(axis) for axis in axes]
    width = [lax.axis_size(axis) * cells for axis, cells in zip(axes, (CX, CY, CZ))]
    at_y = lax.rem(place[1] * CY + lane_index() - 1 + width[1], width[1])
    return place, width, at_y < 2


def floor_of(at_x, width_x, low_y):
    outlet = (at_x >= width_x // 4) & (at_x < width_x - width_x // 4)
    return jnp.where(low_y & jnp.logical_not(outlet), 0.0, -FAR)


def bounds_z(at_z, depth_z):
    return jnp.where(at_z < 2, 0.0, -FAR), jnp.where(at_z >= depth_z - 2, 0.0, FAR)


def velocities(parts, floor, bounds):
    inverse = 1.0 / (parts[3] + mass_floor)
    u_x = parts[0] * inverse
    u_y = jnp.maximum(parts[1] * inverse - time_step * gravity, floor)
    u_z = parts[2] * inverse
    if bounds is not None:
        u_z = jnp.minimum(jnp.maximum(u_z, bounds[0]), bounds[1])
    return u_x, u_y, u_z


def settle_plane(source_ref, source_row, u_ref, step, out_ref, out_step, spot=None):
    spot = step if spot is None else spot
    place, width, low_y = place_bounds()
    sublane = lax.broadcasted_iota(jnp.int32, (8, BLOCK), 0)
    at_x = lax.rem(place[0] * CX + step - 1 + width[0], width[0])
    floor = floor_of(at_x, width[0], low_y)
    for group in range(CZ // 8):
        start = 4 + 32 * group
        parts = [
            source_ref[pl.ds(source_row + start + channel, 8, stride=4), :] for channel in range(4)
        ]
        bounds = None
        if group in (0, CZ // 8 - 1):
            bounds = bounds_z(place[2] * CZ + 8 * group + sublane, width[2])
        values = velocities(parts, floor, bounds)
        for channel in range(3):
            u_ref[pl.ds(spot * PLANE + start + channel, 8, stride=4), :] = values[channel]
            if out_step is not None:
                out_ref[channel, out_step, 8 * group : 8 * group + 8, :] = roll(
                    values[channel], -1
                )[:, 0:CY]


def settle_edges(source_ref, source_row, u_ref, first, count, spot=None):
    spot = first if spot is None else spot
    place, width, low_y = place_bounds()
    sublane = lax.broadcasted_iota(jnp.int32, (8, BLOCK), 0)
    at_x = lax.rem(place[0] * CX + first + sublane - 1 + width[0], width[0])
    floor = floor_of(at_x, width[0], low_y)
    for edge in (0, CZ + 1):
        at_z = lax.rem(place[2] * CZ + edge - 1 + width[2], width[2])
        bounds = bounds_z(at_z + 0 * sublane, width[2])
        parts = [
            source_ref[pl.ds(source_row + 4 * edge + channel, count, stride=PLANE), :]
            for channel in range(4)
        ]
        values = velocities(parts, floor[0:count], [bound[0:count] for bound in bounds])
        for channel in range(3):
            start = spot * PLANE + 4 * edge + channel
            u_ref[pl.ds(start, count, stride=PLANE), :] = values[channel]


def settle_kernel(
    source_ref, grid_ref, spread_ref, out_ref, matrix_ref, edge_ref, u_ref
):
    rim = rim_lanes(lane_index())
    for side, start, place in ((1, 0, 0), (0, CX, 2)):
        for part, tiles in enumerate(unpack_pairs(source_ref, FACE, side * (FACE + 1))):
            for spot, value in enumerate(tiles):
                mine = grid_ref[tile_rows((start + part) * FACE + spot), :]
                if 0 < spot < FACE - 1:
                    mine = mine + jnp.where(rim, 0.0, value)
                edge_ref[tile_rows((place + part) * FACE + spot), :] = mine

    def plane(step, carry):
        row = pl.multiple_of(step * PLANE, 8)
        settle_plane(grid_ref, row, u_ref, step, out_ref, step - 1)
        return carry

    matrix_ref[...] = expansion()
    lax.fori_loop(2, CX, plane, 0, unroll=7)
    for first in range(2, CX, 8):
        count = min(8, CX - first)
        settle_edges(grid_ref, first * PLANE, u_ref, first, count)

    def spread(step, carry):
        row = pl.multiple_of(step * PLANE, 8)
        expand(u_ref[pl.ds(row, PLANE), :], matrix_ref[...], spread_ref, row)
        return carry

    lax.fori_loop(2, CX, spread, 0, unroll=7)


def weights_kernel(blocks, frac_ref, offset_ref, x_ref, z_ref, y_ref):
    for block in range(blocks):
        lanes = slice(block * BLOCK, (block + 1) * BLOCK)
        fraction, offset = point_rows(frac_ref, offset_ref, lanes)
        for side, values in enumerate(lane_weights(fraction[0], offset[0])):
            x_ref[tile_rows(2 * block + side), :] = values
        weight_z, first_z = pair_weights(fraction[2], offset[2])
        for spot, values in enumerate(weight_z + first_z):
            z_ref[tile_rows(6 * block + spot), :] = values
        plain, moment = spline(fraction[1])
        slot = lax.broadcasted_iota(jnp.int32, (8, BLOCK), 0)
        pieces = []
        for group in range(3):
            row = slot + 8 * group
            masks = slot_masks(jnp.where(row < PARTS, row % 6, -100), offset[1])
            values = jnp.concatenate([pick(masks, plain), pick(masks, moment)], axis=1)
            high, low = split(values)
            wide = lax.broadcasted_iota(jnp.int32, values.shape, 0) + 8 * group
            pieces.append(
                jnp.where(wide < 12, high.astype(jnp.float32), low.astype(jnp.float32))
            )
        pieces.append(jnp.zeros_like(pieces[0]))
        y_ref[32 * block : 32 * block + 32, :] = jnp.concatenate(pieces, axis=0).astype(
            jnp.bfloat16
        )


def collect_kernel(
    blocks,
    tile_vmem,
    late_ref,
    x_ref,
    z_ref,
    y_ref,
    early_ref,
    inner_ref,
    matrix_ref,
    _,
    spread_ref,
    out_hbm,
    velocity_hbm,
    affine_hbm,
    edge_ref,
    u_ref,
    out_ref,
    stage_ref,
    velocity_ref,
    affine_ref,
    tile_ref,
    sems,
):
    tile_copy = pltpu.make_async_copy(tile_vmem, tile_ref, sems.at[3 + 2 * (blocks // CHUNK)])
    tile_copy.start()
    inner = pltpu.make_async_copy(
        inner_ref.at[:, pl.ds(1, CX - 2)], out_hbm.at[:, pl.ds(1, CX - 2)], sems.at[2]
    )
    inner.start()
    for side, place in ((1, 0), (0, 2)):
        for part, tiles in enumerate(late_planes(late_ref, 3 * side)):
            for spot, value in enumerate(tiles):
                rows = tile_rows((place + part) * FACE + spot)
                edge_ref[rows, :] = early_ref[rows, :] + value
    for spot, step in enumerate((0, 1, CX, CX + 1)):
        out_step = {1: 0, CX: 1}.get(step)
        settle_plane(edge_ref, spot * PLANE, u_ref, step, out_ref, out_step, spot)
    settle_edges(edge_ref, 0, u_ref, 0, 2)
    settle_edges(edge_ref, 2 * PLANE, u_ref, CX, 2, 2)
    matrix = matrix_ref[...]
    for spot, step in ((0, 0), (2, CX)):
        values = u_ref[spot * PLANE : (spot + 2) * PLANE, :]
        expand(values, matrix, spread_ref, step * PLANE)
    copies = [
        pltpu.make_async_copy(
            out_ref.at[:, pl.ds(slot, 1)],
            out_hbm.at[:, pl.ds(slot * (CX - 1), 1)],
            sems.at[slot],
        )
        for slot in range(2)
    ]
    for copy in copies:
        copy.start()
    copies.append(inner)

    def one_block(block):
        lanes = pl.ds(pl.multiple_of(block * BLOCK, BLOCK), BLOCK)
        corner, corner_y = tile_corner(tile_ref[block])

        def x_row(slot):
            return x_ref[pl.ds(block * 16 + slot, 8, stride=0), :]

        def z_tile(slot):
            return z_ref[pl.ds(pl.multiple_of(block * 48 + 8 * slot, 8), 8), :]

        weight_x = [x_row(slot) for slot in range(6)]
        first_x = [x_row(8 + slot) for slot in range(6)]
        weight_z = [z_tile(slot) for slot in range(3)]
        first_z = [z_tile(3 + slot) for slot in range(3)]
        right = y_ref[pl.ds(pl.multiple_of(block * 32, 32), 32), :]
        seat = corner_y // 4
        spread = seat // SEATS
        corner = corner + spread * (PX * PLANE)
        turn = (128 - PARTS * (seat - spread * SEATS)) & 127
        left = jnp.concatenate(
            [pltpu.roll(spread_ref[window_rows(corner, step), :], turn, 1) for step in range(6)],
            axis=0,
        ).astype(jnp.bfloat16)

        sums = jnp.dot(left[:, 0:24], right[0:24], preferred_element_type=jnp.float32)

        def over_x(weights, column):
            result = []
            for pair in range(3):
                total = None
                for step in range(6):
                    row = 24 * step + 8 * pair
                    term = weights[step] * sums[row : row + 8, column : column + BLOCK]
                    total = term if total is None else total + term
                result.append(total)
            return result

        def over_z(weights, values):
            total = weights[0] * values[0] + weights[1] * values[1] + weights[2] * values[2]
            return total + pltpu.roll(total, 4, 0)

        plain = over_x(weight_x, 0)
        velocity = over_z(weight_z, plain)
        columns = (
            over_z(weight_z, over_x(first_x, 0)),
            over_z(weight_z, over_x(weight_x, BLOCK)),
            over_z(first_z, plain),
        )
        return block, lanes, velocity, columns

    chunk_count = blocks // CHUNK
    tile_copy.wait()

    def chunk_copies(chunk):
        part = pl.ds(pl.multiple_of(chunk * (CHUNK * BLOCK), BLOCK), CHUNK * BLOCK)
        return [
            pltpu.make_async_copy(
                source.at[:, part], target.at[:, part], sems.at[3 + side * chunk_count + chunk]
            )
            for side, (source, target) in enumerate(
                ((velocity_ref, velocity_hbm), (affine_ref, affine_hbm))
            )
        ]

    def one_chunk(chunk, carry):
        results = [one_block(chunk * CHUNK + spot) for spot in range(CHUNK)]
        for block, lanes, velocity, columns in results:
            velocity_ref[:, lanes] = velocity[0:3]
            for col in range(3):
                stage_ref[pl.ds(block * 16 + col, 3, stride=3), :] = 4.0 * columns[col][0:3]
        for block, lanes, _, _ in results:
            affine_ref[:, lanes] = stage_ref[pl.ds(pl.multiple_of(block * 16, 8), 9), :]
        for copy in chunk_copies(chunk):
            copy.start()
        return carry

    lax.fori_loop(0, chunk_count, one_chunk, 0, unroll=min(chunk_count, 4))
    for chunk in range(chunk_count):
        copies += chunk_copies(chunk)
    for copy in copies:
        copy.wait()


def exchange(low, high, axis):
    count = lax.axis_size(axis)
    up = [(i, (i + 1) % count) for i in range(count)]
    down = [(target, source) for source, target in up]
    above = lax.ppermute(low, axis, down)
    below = lax.ppermute(high, axis, up)
    return above, below


def exchange_both(message, axis):
    if lax.axis_size(axis) == 2:
        return lax.ppermute(message, axis, [(0, 1), (1, 0)])
    half = message.shape[0] // 2
    return jnp.concatenate(exchange(message[:half], message[half:], axis))


def step(
    point_frac,
    cell_offset,
    point_velocity,
    point_affine,
    point_stress,
    point_mass,
    block_tile,
    block_count,
):
    blocks = block_tile.shape[0]
    points = blocks * BLOCK
    f32 = jnp.float32
    vmem = pl.BlockSpec(memory_space=pltpu.VMEM)
    hbm = pl.BlockSpec(memory_space=pltpu.HBM)
    params = pltpu.CompilerParams(vmem_limit_bytes=VMEM_LIMIT)
    grid_shape = jax.ShapeDtypeStruct((ROWS, BLOCK), f32)
    out_shape = jax.ShapeDtypeStruct((3, CX, CZ, CY), f32)

    def message(tiles):
        return jax.ShapeDtypeStruct((8 * tiles, BLOCK), f32)

    def cost(microseconds):
        return pl.CostEstimate(
            flops=int(microseconds * 8.0e6), bytes_accessed=1000, transcendentals=0
        )

    mass = point_mass.reshape(blocks, BLOCK)
    inputs = (
        block_tile,
        block_count,
        point_frac,
        cell_offset,
        point_velocity,
        point_affine,
        point_stress,
        mass,
    )
    new_stress, grid, low, high = pl.pallas_call(
        lambda *refs: deposit_kernel(blocks, *refs),
        out_shape=(
            jax.ShapeDtypeStruct((6, points), f32),
            grid_shape,
            message(PX // 2 + 1),
            message(PX // 2 + 1),
        ),
        in_specs=[hbm] * 8,
        out_specs=(hbm,) + (vmem,) * 3,
        scratch_shapes=[
            pltpu.SMEM(block_tile.shape, jnp.int32),
            pltpu.SMEM(block_count.shape, jnp.int32),
        ]
        + [pltpu.VMEM(array.shape, array.dtype) for array in inputs[2:]]
        + [
            pltpu.VMEM((6, points), f32),
            pltpu.VMEM((50 * STRIDE, BLOCK), f32),
            pltpu.SemaphoreType.DMA((9,)),
        ],
        compiler_params=params,
        cost_estimate=cost(5),
        name="deposit",
    )(*[pltpu.with_memory_space_constraint(array, pltpu.HBM) for array in inputs])
    weigh = pl.pallas_call(
        lambda *refs: weights_kernel(blocks, *refs),
        out_shape=(
            message(2 * blocks),
            message(6 * blocks),
            jax.ShapeDtypeStruct((32 * blocks, 2 * BLOCK), jnp.bfloat16),
        ),
        in_specs=[vmem] * 2,
        out_specs=(vmem,) * 3,
        compiler_params=params,
        cost_estimate=cost(1),
        name="weights",
    )
    weights = weigh(point_frac, cell_offset)
    above, below = exchange(low, high, "gz")
    pack = pl.pallas_call(
        pack_kernel,
        out_shape=(message(SPAN), message(SPAN), message(2 * (FACE + 1))),
        in_specs=[vmem],
        out_specs=(vmem,) * 3,
        compiler_params=params,
        cost_estimate=cost(0.5),
        name="pack_y",
    )
    low, high, early = pack(grid)
    early = exchange_both(early, "gx")
    grid, low, high = pl.pallas_call(
        join_z,
        out_shape=(grid_shape, message(SPAN), message(SPAN)),
        in_specs=[vmem] * 5,
        out_specs=(vmem,) * 3,
        input_output_aliases={4: 0},
        compiler_params=params,
        cost_estimate=cost(0.3),
        name="join_z",
    )(above, below, low, high, grid)
    above, below = exchange(low, high, "gy")
    weigh = pl.pallas_call(
        lambda *refs: weights_kernel(blocks, *refs),
        out_shape=(
            message(2 * blocks),
            message(6 * blocks),
            jax.ShapeDtypeStruct((32 * blocks, 2 * BLOCK), jnp.bfloat16),
        ),
        in_specs=[vmem] * 2,
        out_specs=(vmem,) * 3,
        compiler_params=params,
        cost_estimate=cost(1),
        name="weights",
    )
    weights = weigh(point_frac, cell_offset)
    grid, late = pl.pallas_call(
        join_y_edges,
        out_shape=(grid_shape, message(6)),
        in_specs=[vmem] * 3,
        out_specs=(vmem,) * 2,
        input_output_aliases={2: 0},
        compiler_params=params,
        cost_estimate=cost(0.3),
        name="join_y_edges",
    )(above, below, grid)
    rest = pl.pallas_call(
        join_y_rest,
        out_shape=grid_shape,
        in_specs=[vmem] * 3,
        out_specs=vmem,
        input_output_aliases={2: 0},
        compiler_params=params,
        cost_estimate=cost(1),
        name="join_y_rest",
    )
    grid = rest(above, below, grid)
    late = exchange_both(late, "gx")
    spread_shape = message(SPREADS * TILES)
    spread, inner, matrix, edge = pl.pallas_call(
        settle_kernel,
        out_shape=(
            spread_shape,
            out_shape,
            jax.ShapeDtypeStruct((2 * BLOCK, SPREADS * BLOCK), jnp.bfloat16),
            message(4 * FACE),
        ),
        in_specs=[vmem] * 2,
        out_specs=(vmem,) * 4,
        scratch_shapes=[pltpu.VMEM((PX * PLANE, BLOCK), f32)],
        compiler_params=params,
        cost_estimate=cost(2),
        name="settle",
    )(early, grid)
    _, grid_velocity, new_velocity, new_affine = pl.pallas_call(
        lambda *refs: collect_kernel(blocks, *refs),
        out_shape=(
            spread_shape,
            out_shape,
            jax.ShapeDtypeStruct((3, points), f32),
            jax.ShapeDtypeStruct((9, points), f32),
        ),
        in_specs=[vmem] * 9,
        out_specs=(vmem, hbm, hbm, hbm),
        input_output_aliases={8: 0},
        scratch_shapes=[
            pltpu.VMEM((4 * PLANE, BLOCK), f32),
            pltpu.VMEM((4 * PLANE, BLOCK), f32),
            pltpu.VMEM((3, 2, CZ, CY), f32),
            pltpu.VMEM((blocks * 16, BLOCK), f32),
            pltpu.VMEM((3, points), f32),
            pltpu.VMEM((9, points), f32),
            pltpu.SMEM(block_tile.shape, jnp.int32),
            pltpu.SemaphoreType.DMA((4 + 2 * (blocks // CHUNK),)),
        ],
        compiler_params=params,
        cost_estimate=cost(4),
        name="collect",
    )(block_tile, late, *weights, edge, inner, matrix, spread)
    return (new_velocity, new_affine, new_stress, grid_velocity.transpose(0, 1, 3, 2))


def solution(mesh):
    points = ("gx", "gy", "gz")
    return jax.shard_map(
        step,
        mesh=mesh,
        in_specs=(P(None, points),) * 5 + (P(points),) * 3,
        out_specs=(P(None, points),) * 3 + (P(None, "gx", "gy", "gz"),),
        check_vma=False,
    )
```
